32 devices in a mesh: dp: 4 (over x, y), sp: 8 (over z, core).
Axes of the slice: x: 2, y: 2, z: 4, core: 2. Of those that a mesh axis runs over, the one named last changes fastest.
Arguments:
- x: bfloat16 [16384, 4096], P(('dp', 'sp')), parts along dimension 0
- gain: bfloat16 [4096], replicated
- wq: bfloat16 [4096, 4096], P('sp')
- wk: bfloat16 [4096, 1024], P('sp')
- wv: bfloat16 [4096, 1024], P('sp')
- wo: bfloat16 [4096, 4096], P('sp')
Outputs:
- output: bfloat16 [16384, 4096], P(('dp', 'sp')), parts along dimension 0
There are 4 independent parts. The reference program is written for one: setup_inputs(seed, part) draws one part's arguments, and reference() takes and returns one part's arrays. A program takes and returns all parts, laid end to end along the dimension named above; an argument that names none is the same for every part.
All inputs are finite; a program needn't handle non-finite values.
Results may differ from the reference program's by a relative error of at most 0.012.
Values are sent between devices in bfloat16 or wider.
A program may use at most 2 GiB of HBM per device.

```python
import jax
import jax.numpy as jnp
from jax import lax

ROWS = 4096
D = 4096
HEADS = 32
KV_HEADS = 8
HEAD = 128
THETA = 10000


def setup_inputs(seed: int = 0, part: int = 0) -> dict:
    kx, kn, kq, kk, kv, ko = jax.random.split(jax.random.key(seed), 6)

    def weights(key, rows, columns):
        return jax.random.normal(key, (rows, columns), jnp.float32) * rows**-0.5

    drawn = {
        "x": jax.random.normal(jax.random.fold_in(kx, part), (ROWS, D), jnp.float32),
        "gain": 1 + 0.1 * jax.random.normal(kn, (D,), jnp.float32),
        "wq": 2 * weights(kq, D, HEADS * HEAD),
        "wk": 2 * weights(kk, D, KV_HEADS * HEAD),
        "wv": 4 * weights(kv, D, KV_HEADS * HEAD),
        "wo": weights(ko, HEADS * HEAD, D),
    }
    return {k: v.astype(jnp.bfloat16) for k, v in drawn.items()}


def normed(x, gain):
    wide = x.astype(jnp.float32)
    scale = lax.rsqrt(jnp.mean(wide * wide, -1, keepdims=True) + 1e-6)
    return (wide * scale * gain.astype(jnp.float32)).astype(jnp.bfloat16)


def turned(t, place, theta):
    half = t.shape[-1] // 2
    angle = place.astype(jnp.float32)[:, None] * theta ** (-jnp.arange(half, dtype=jnp.float32) / half)
    cos, sin = jnp.cos(angle)[:, None], jnp.sin(angle)[:, None]
    a, b = t[..., :half].astype(jnp.float32), t[..., half:].astype(jnp.float32)
    return jnp.concatenate([a * cos - b * sin, b * cos + a * sin], -1).astype(jnp.bfloat16)


def matmul(a, w):
    return jnp.dot(a, w, preferred_element_type=jnp.float32).astype(jnp.bfloat16)


def einsum(form, a, b):
    return jnp.einsum(form, a.astype(jnp.float32), b.astype(jnp.float32))


def attention(q, k, v):
    scores = einsum("tgsd,ugd->gstu", q, k) * q.shape[-1] ** -0.5
    token = jnp.arange(q.shape[0])
    scores = jnp.where(token[:, None] >= token, scores, -jnp.inf)
    weights = jax.nn.softmax(scores, -1).astype(jnp.bfloat16)
    return einsum("gstu,ugd->tgsd", weights, v).astype(jnp.bfloat16)


def reference(x, gain, wq, wk, wv, wo):
    a, place = normed(x, gain), jnp.arange(ROWS)
    q = turned(matmul(a, wq).reshape(ROWS, HEADS, HEAD), place, THETA).reshape(ROWS, KV_HEADS, -1, HEAD)
    k = turned(matmul(a, wk).reshape(ROWS, KV_HEADS, HEAD), place, THETA)
    v = matmul(a, wv).reshape(ROWS, KV_HEADS, HEAD)
    seen = attention(q, k, v).reshape(ROWS, HEADS * HEAD)
    return (x.astype(jnp.float32) + jnp.dot(seen, wo, preferred_element_type=jnp.float32)).astype(jnp.bfloat16)
```

```python
import functools

import jax
import jax.numpy as jnp
from jax import lax
from jax.experimental import pallas as pl
from jax.experimental.pallas import tpu as pltpu
from jax.sharding import PartitionSpec as P

HEAD = 128
THETA = 10000
NEG = -1e30
HIDDEN = 2 * NEG
LOG2E = 1.4426950408889634
MESH = pl.DeviceIdType.MESH
BF = jnp.bfloat16
F32 = jnp.float32

T = 1024
D = 4096
H = 512
QR = 128
WIDE = (1024, 2048, 2048)
KV, Q, O = 0, 1, 2
KB = 512
STRIP = 512


def _dot(a, b, ca, cb):
    return lax.dot_general(a, b, (((ca,), (cb,)), ((), ())), preferred_element_type=F32)


def _layer(x_ref, gain_ref, wq_ref, wk_ref, wv_ref, wo_ref, cos_ref, sin_ref, y_ref, xp_ref, bkv, bq, bo, xa, wst, acc, q_s, ks, vs, mix_s,
           top_s, so, sf, zr, fs, fr, cs, cr, ps, pr, hs, hr, ys, yr, ld, xl, rdy):
    dp, sp = lax.axis_index("dp"), lax.axis_index("sp")
    z, c = sp // 2, sp % 2
    jx, jy = dp // 2, dp % 2
    xd, yd, diag = (1 - jx) * 2 + jy, jx * 2 + 1 - jy, 3 - dp
    half = z // 2
    inner = z + half * (3 - 2 * z)
    mid = inner == 1
    partner = z * 2 + 1 - c
    bufs = (bkv, bq, bo)

    def remote(src, dst, send, recv, d, s):
        return pltpu.make_async_remote_copy(src_ref=src, dst_ref=dst, send_sem=send, recv_sem=recv, device_id={"dp": d, "sp": s}, device_id_type=MESH)

    def lanes(i, n):
        return pl.ds(pl.multiple_of(i * n, n), n)

    def rows(i, n):
        return pl.ds(pl.multiple_of(i * n, n), n)

    def origin(r):
        base = (1 - inner, 2, 3)[r - 1]
        return base + half * (3 - 2 * base)

    def mine(m, cc):
        if m == KV:
            return [(wk_ref, lanes(cc, 512), pl.ds(0, 512)), (wv_ref, lanes(cc, 512), pl.ds(512, 512))]
        return [((None, wq_ref, wo_ref)[m], lanes(cc, 2048), pl.ds(0, 2048))]

    def own_copies(m, d, cc):
        return [remote(w.at[rows(dp, QR), cols], bufs[m].at[2 * z + c, rows(dp, QR), at], so.at[m, d, cc], zr.at[m, z, c], dp, (z + (1, -1)[d]) * 2 + cc)
                for w, cols, at in mine(m, cc)]

    def own_sends(m):
        for d in (0, 1):
            @pl.when((z < 3) if d == 0 else (z > 0))
            def _():
                for cc in (0, 1):
                    for cp in own_copies(m, d, cc):
                        cp.start()

    def zfwd(m, r, cc):
        o = origin(r)
        step = (1 if r == 1 else -1) * (1 - 2 * half)
        part = bufs[m].at[2 * o + cc, rows(dp, QR)]
        return remote(part, part, sf.at[m, r - 1, cc], zr.at[m, o, cc], dp, (z + step) * 2 + c)

    def zwait(m, r):
        for cc in (0, 1):
            zfwd(m, r, cc).wait_recv()

    def zforward(m, r):
        @pl.when(mid)
        def _():
            for cc in (0, 1):
                zfwd(m, r, cc).start()

    def plane(m, r, k):
        o, b = origin(r), bufs[m]
        part = (b.at[pl.ds(2 * o, 2), rows(dp, QR)], b.at[pl.ds(2 * o, 2), rows(dp, QR)], b.at[2 * o, rows(xd, QR)], b.at[2 * o + 1, rows(yd, QR)])[k]
        return remote(part, part, fs.at[m, r - 1, k], fr.at[m, r - 1, k], (xd, yd, yd, xd)[k], sp)

    def plane_in(m, r, k):
        o, b = origin(r), bufs[m]
        part = (b.at[pl.ds(2 * o, 2), rows(xd, QR)], b.at[pl.ds(2 * o, 2), rows(yd, QR)], b.at[2 * o, rows(diag, QR)], b.at[2 * o + 1, rows(diag, QR)])[k]
        return remote(part, part, fs.at[m, r - 1, k], fr.at[m, r - 1, k], (xd, yd, yd, xd)[k], sp)

    def xyforward(m, r):
        plane(m, r, 0).start()
        plane(m, r, 1).start()

    def second(m, r):
        plane_in(m, r, 0).wait_recv()
        plane_in(m, r, 1).wait_recv()
        plane(m, r, 2).start()
        plane(m, r, 3).start()

    def third(m, r):
        plane_in(m, r, 2).wait_recv()
        plane_in(m, r, 3).wait_recv()

    def first(m, r):
        zwait(m, r)
        zforward(m, r)
        xyforward(m, r)

    def shared(m):
        return [remote(w.at[:, cols], bufs[m].at[2 * z + c, :, at], ps.at[2 + m], pr.at[2 + m], dp, partner) for w, cols, at in mine(m, 1 - c)]

    def shared_wait(m):
        part = bufs[m].at[2 * z + 1 - c]
        remote(part, part, ps.at[2 + m], pr.at[2 + m], dp, partner).wait_recv()

    x_near = pltpu.make_async_copy(x_ref, xa.at[rows(c, H)], xl.at[0])
    x_far = remote(x_ref, xa.at[rows(c, H)], ps.at[0], pr.at[0], dp, partner)
    x_rest = remote(x_ref.at[:, lanes(1 - c, 2048)], xp_ref, ps.at[1], pr.at[1], dp, partner)

    def loads(m, r, slot):
        if r == 0:
            near = [pltpu.make_async_copy(w.at[:, cols], wst.at[slot, rows(c, H), at], ld.at[slot, i]) for i, (w, cols, at) in enumerate(mine(m, c))]
            return near + [pltpu.make_async_copy(bufs[m].at[2 * z + 1 - c], wst.at[slot, rows(1 - c, H), pl.ds(0, WIDE[m])], ld.at[slot, 2])]
        o = origin(r)
        return [pltpu.make_async_copy(bufs[m].at[2 * o + i], wst.at[slot, pl.ds(i * H, H), pl.ds(0, WIDE[m])], ld.at[slot, i]) for i in (0, 1)]

    def load(m, r, slot):
        for cp in loads(m, r, slot):
            cp.start()

    def loaded(m, r, slot):
        for cp in loads(m, r, slot):
            cp.wait()

    def part(r):
        return lanes(z if r == 0 else origin(r), T)

    def multiply(m, r, slot):
        depth = part(r)

        @pl.loop(0, WIDE[m] // 256)
        def _(i):
            cols = lanes(i, 256)
            w = wst[slot, :, cols]
            for j in (0, 1):
                at = pl.ds(j * H, H)
                got = _dot(xa[at, depth], w, 1, 0)
                if r == 0:
                    acc[at, cols] = got
                else:
                    acc[at, cols] += got

    def project(m, r, slot):
        load(m, r, slot)
        loaded(m, r, slot)
        multiply(m, r, slot)

    def turned(t):
        t = t.astype(BF).astype(F32)
        return (t * cos_ref[...] + pltpu.roll(t, HEAD // 2, 1) * sin_ref[...]).astype(BF)

    def kv_out(d):
        o = z - d
        return [remote(b.at[o], b.at[o], cs.at[d, i], cr.at[d, i], dp, sp + 2) for i, b in enumerate((ks, vs))]

    def kv_in(d):
        o = z - d
        return [remote(b.at[o], b.at[o], cs.at[d - 1, i], cr.at[d - 1, i], dp, sp) for i, b in enumerate((ks, vs))]

    def kv_forward(d):
        @pl.when(z >= d)
        def _():
            for cp in kv_in(d):
                cp.wait_recv()

            @pl.when(z < 3)
            def _():
                for cp in kv_out(d):
                    cp.start()

    e = HEAD**-0.5 * LOG2E

    def block(o, g, keys, strips, fresh):
        k = ks[o, g, keys, :]
        scores = [_dot(k, q_s[g, at : at + STRIP, :], 1, 1) for at, _ in strips]
        values = jnp.concatenate([vs[o, g, :, keys], jnp.ones((8, KB), BF)], axis=0)
        weights, keeps = [], []
        for (at, gap), s in zip(strips, scores):
            if gap is not None:
                ok = lax.broadcasted_iota(jnp.int32, (KB, STRIP), 1) + gap >= lax.broadcasted_iota(jnp.int32, (KB, STRIP), 0)
                s = jnp.where(ok, s, HIDDEN)
            top = s.max(axis=0, keepdims=True)
            if not fresh:
                old = top_s[g, :, at : at + STRIP]
                top = jnp.maximum(old, top)
                keeps.append(jnp.exp2((old - top) * e))
            top_s[g, :, at : at + STRIP] = top
            weights.append(jnp.exp2((s - top) * e).astype(BF))
        for i, ((at, _), p) in enumerate(zip(strips, weights)):
            got = _dot(values, p, 1, 0)
            if fresh:
                mix_s[g, :, at : at + STRIP] = got
            else:
                mix_s[g, :, at : at + STRIP] = mix_s[g, :, at : at + STRIP] * keeps[i] + got

    def attend_own():
        @pl.loop(0, 4)
        def _(g):
            block(z, g, pl.ds(0, KB), [(at, 0 if at % T == 0 else None) for at in range(0, 4 * T, STRIP)], True)
            block(z, g, pl.ds(KB, KB), [(at, 0) for at in range(STRIP, 4 * T, T)], False)

    def attend(d):
        @pl.loop(0, 8)
        def _(i):
            block(z - d, i // 2, lanes(i % 2, KB), [(at, None) for at in range(0, 4 * T, STRIP)], False)

    def seen_copy(g):
        cols = lanes(c * 4 + g, 512)
        return remote(xa.at[:, cols], xa.at[:, cols], hs.at[g], hr.at[g], dp, partner)

    def seen_in(g):
        cols = lanes((1 - c) * 4 + g, 512)
        return remote(xa.at[:, cols], xa.at[:, cols], hs.at[g], hr.at[g], dp, partner)

    barrier = pltpu.get_barrier_semaphore()
    greeted = [(dp, partner), (xd, sp), (yd, sp)]
    for d, s in greeted:
        pl.semaphore_signal(barrier, inc=1, device_id={"dp": d, "sp": s}, device_id_type=MESH)
    for near, step in ((z < 3, 1), (z > 0, -1)):
        @pl.when(near)
        def _():
            for cc in (0, 1):
                pl.semaphore_signal(barrier, inc=1, device_id={"dp": dp, "sp": (z + step) * 2 + cc}, device_id_type=MESH)
    pl.semaphore_wait(barrier, len(greeted) + 2 + 2 * inner)

    x_near.start()
    x_far.start()
    own_sends(KV)
    for m in (KV, Q):
        for cp in shared(m):
            cp.start()
    x_near.wait()
    x_far.wait_recv()

    @pl.loop(0, T // 32)
    def _(i):
        at = rows(i, 32)
        wide = xa[at, :].astype(F32)
        scale = lax.rsqrt(jnp.mean(wide * wide, -1, keepdims=True) + 1e-6)
        xa[at, :] = (wide * scale * gain_ref[...].astype(F32)).astype(BF)

    shared_wait(KV)
    project(KV, 0, 0)
    first(KV, 1)
    first(KV, 2)
    second(KV, 1)
    first(KV, 3)
    own_sends(Q)
    second(KV, 2)
    second(KV, 3)
    third(KV, 1)
    project(KV, 1, 1)
    third(KV, 2)
    project(KV, 2, 0)
    first(Q, 1)
    third(KV, 3)
    project(KV, 3, 1)
    for g in range(4):
        ks[z, g] = turned(acc[:, g * HEAD : (g + 1) * HEAD])
        vs[z, g] = acc[:, 512 + g * HEAD : 512 + (g + 1) * HEAD].T.astype(BF)

    @pl.when(mid)
    def _():
        for r in (2, 3):
            zwait(Q, r)
    for r in (2, 3):
        zforward(Q, r)

    @pl.when(z < 3)
    def _():
        for cp in kv_out(0):
            cp.start()
    own_sends(O)
    x_rest.start()
    for cp in shared(O):
        cp.start()
    shared_wait(Q)
    project(Q, 0, 0)
    for r in (2, 3):
        @pl.when(inner == 0)
        def _():
            zwait(Q, r)
        xyforward(Q, r)
        second(Q, r - 1)
        third(Q, r - 1)
        project(Q, r - 1, 1 if r == 2 else 0)
    second(Q, 3)
    kv_forward(1)
    first(O, 1)
    third(Q, 3)
    project(Q, 3, 1)
    pl.semaphore_signal(rdy, inc=1, device_id={"dp": dp, "sp": partner}, device_id_type=MESH)

    @pl.loop(0, 4)
    def _(g):
        for n in range(4):
            q_s[g, n * T : (n + 1) * T, :] = turned(acc[:, lanes(g * 4 + n, HEAD)])

    attend_own()

    @pl.when(z == 2)
    def _():
        kv_forward(2)

    second(O, 1)

    def rest(d):
        @pl.when(z >= d)
        def _():
            attend(d)

    rest(1)

    @pl.when(z == 3)
    def _():
        kv_forward(2)
    first(O, 2)
    rest(2)
    second(O, 2)
    kv_forward(3)
    rest(3)
    first(O, 3)

    pl.semaphore_wait(rdy, 1)

    @pl.loop(0, 4)
    def _(g):
        for n in range(4):
            at = slice(n * T, (n + 1) * T)
            out = mix_s[g, :HEAD, at] * (1 / mix_s[g, HEAD : HEAD + 1, at])
            xa[:, lanes(c * 16 + g * 4 + n, HEAD)] = out.T.astype(BF)
    for g in range(4):
        seen_copy(g).start()
    shared_wait(O)
    load(O, 0, 0)
    third(O, 1)
    load(O, 1, 1)
    for g in range(4):
        seen_in(g).wait_recv()
    loaded(O, 0, 0)
    multiply(O, 0, 0)
    second(O, 3)
    third(O, 2)
    load(O, 2, 0)
    loaded(O, 1, 1)
    multiply(O, 1, 1)
    loaded(O, 2, 0)
    multiply(O, 2, 0)
    x_rest.wait_recv()
    rest_x = [pltpu.make_async_copy(x_ref.at[:, lanes(c, 2048)], wst.at[0, rows(c, H)], xl.at[1]),
              pltpu.make_async_copy(xp_ref, wst.at[0, rows(1 - c, H)], xl.at[2])]
    for cp in rest_x:
        cp.start()
    third(O, 3)
    load(O, 3, 1)
    for cp in rest_x:
        cp.wait()
    loaded(O, 3, 1)

    def results(i):
        cols, to = pl.ds(i * 512, 512), lanes(c * 4 + i, 512)
        return (pltpu.make_async_copy(wst.at[0, rows(c, H), cols], y_ref.at[:, to], xl.at[3 + i]),
                remote(wst.at[0, rows(1 - c, H), cols], y_ref.at[:, to], ys.at[i], yr.at[i], dp, partner))

    def result_in(i):
        to = lanes((1 - c) * 4 + i, 512)
        return remote(y_ref.at[:, to], y_ref.at[:, to], ys.at[i], yr.at[i], dp, partner)

    depth = part(3)
    for i in range(4):
        for n in (0, 1):
            cols = slice(i * 512 + n * 256, i * 512 + n * 256 + 256)
            for j in (0, 1):
                at = slice(j * H, (j + 1) * H)
                got = acc[at, cols] + _dot(xa[at, depth], wst[1, :, cols], 1, 0)
                wst[0, at, cols] = (wst[0, at, cols].astype(F32) + got).astype(BF)
        for cp in results(i):
            cp.start()

    for i in range(4):
        near, far = results(i)
        near.wait()
        far.wait_send()
        result_in(i).wait_recv()
        seen_copy(i).wait_send()
    x_far.wait_send()
    x_rest.wait_send()
    for m in (KV, Q, O):
        here = bufs[m].at[2 * z + c]
        remote(here, here, ps.at[2 + m], pr.at[2 + m], dp, partner).wait_send()
        quarter = bufs[m].at[2 * z + c, rows(dp, QR)]
        for d in (0, 1):
            @pl.when((z < 3) if d == 0 else (z > 0))
            def _():
                for cc in (0, 1):
                    remote(quarter, quarter, so.at[m, d, cc], zr.at[m, z, c], dp, (z + (1, -1)[d]) * 2 + cc).wait_send()
        for r in (1, 2, 3):
            @pl.when(mid)
            def _():
                for cc in (0, 1):
                    zfwd(m, r, cc).wait_send()
            for k in range(4):
                plane(m, r, k).wait_send()
    for d in (0, 1, 2):
        @pl.when((z >= d) & (z < 3))
        def _():
            for cp in kv_out(d):
                cp.wait_send()


def solution(mesh):
    def step(x, gain, wq, wk, wv, wo):
        place = (lax.axis_index("sp") // 2) * T + jnp.arange(T)
        angle = place.astype(F32)[:, None] * THETA ** (-jnp.arange(HEAD // 2, dtype=F32) / (HEAD // 2))
        cos, sin = jnp.cos(angle), jnp.sin(angle)
        cos, sin = jnp.concatenate([cos, cos], 1), jnp.concatenate([-sin, sin], 1)
        far, near = pl.BlockSpec(memory_space=pl.ANY), pl.BlockSpec(memory_space=pltpu.VMEM)
        sems = pltpu.SemaphoreType.DMA
        y, *_ = pl.pallas_call(
            _layer,
            out_shape=[
                jax.ShapeDtypeStruct((H, D), BF),
                jax.ShapeDtypeStruct((H, 2048), BF),
                *(jax.ShapeDtypeStruct((8, H, n), BF) for n in WIDE),
            ],
            in_specs=[far, near, far, far, far, far, near, near],
            out_specs=[far] * 5,
            scratch_shapes=[
                pltpu.VMEM((T, D), BF),
                pltpu.VMEM((2, T, 2048), BF),
                pltpu.VMEM((T, 2048), F32),
                pltpu.VMEM((4, 4 * T, HEAD), BF),
                pltpu.VMEM((4, 4, T, HEAD), BF),
                pltpu.VMEM((4, 4, HEAD, T), BF),
                pltpu.VMEM((4, HEAD + 8, 4 * T), F32),
                pltpu.VMEM((4, 1, 4 * T), F32),
                sems((3, 2, 2)),
                sems((3, 3, 2)),
                sems((3, 4, 2)),
                sems((3, 3, 4)),
                sems((3, 3, 4)),
                sems((3, 2)),
                sems((3, 2)),
                sems((5,)),
                sems((5,)),
                sems((4,)),
                sems((4,)),
                sems((4,)),
                sems((4,)),
                sems((2, 3)),
                sems((7,)),
                pltpu.SemaphoreType.REGULAR,
            ],
            compiler_params=pltpu.CompilerParams(collective_id=0, has_side_effects=True, vmem_limit_bytes=63 * 2**20),
        )(x, gain[None], wq, wk, wv, wo, cos, sin)
        return y

    tokens, whole = P(("dp", "sp"), None), P("sp", None)
    return jax.shard_map(
        step,
        mesh=mesh,
        in_specs=(tokens, P(None), whole, whole, whole, whole),
        out_specs=tokens,
        check_vma=False,
    )
```

```python
import functools

import jax
import jax.numpy as jnp
from jax import lax
from jax.experimental import pallas as pl
from jax.experimental.pallas import tpu as pltpu
from jax.sharding import PartitionSpec as P

HEAD = 128
THETA = 10000
NEG = -1e30
HIDDEN = 2 * NEG
LOG2E = 1.4426950408889634
MESH = pl.DeviceIdType.MESH
BF = jnp.bfloat16
F32 = jnp.float32

T = 1024
D = 4096
H = 512
QR = 128
W = 1024
KV, Q, O = (0,), (1, 2), (3, 4)
KB = 512
STRIP = 512


def _dot(a, b, ca, cb):
    return lax.dot_general(a, b, (((ca,), (cb,)), ((), ())), preferred_element_type=F32)


def _layer(x_ref, gain_ref, wq_ref, wk_ref, wv_ref, wo_ref, cos_ref, sin_ref, y_ref, xp_ref, b0, b1, b2, b3, b4, xa, wst, acc, q_s, ks, vs, mix_s,
           top_s, so, sf, zr, fs, fr, cs, cr, ps, pr, hs, hr, ys, yr, ld, xl, rdy):
    dp, sp = lax.axis_index("dp"), lax.axis_index("sp")
    z, c = sp // 2, sp % 2
    jx, jy = dp // 2, dp % 2
    xd, yd, diag = (1 - jx) * 2 + jy, jx * 2 + 1 - jy, 3 - dp
    half = z // 2
    inner = z + half * (3 - 2 * z)
    mid = inner == 1
    partner = z * 2 + 1 - c
    bufs = (b0, b1, b2, b3, b4)

    def remote(src, dst, send, recv, d, s):
        return pltpu.make_async_remote_copy(src_ref=src, dst_ref=dst, send_sem=send, recv_sem=recv, device_id={"dp": d, "sp": s}, device_id_type=MESH)

    def lanes(i, n):
        return pl.ds(pl.multiple_of(i * n, n), n)

    def rows(i, n):
        return pl.ds(pl.multiple_of(i * n, n), n)

    def origin(r):
        base = (1 - inner, 2, 3)[r - 1]
        return base + half * (3 - 2 * base)

    def mine(m, cc):
        if m == 0:
            return [(wk_ref, lanes(cc, 512), pl.ds(0, 512)), (wv_ref, lanes(cc, 512), pl.ds(512, 512))]
        return [(wq_ref if m in Q else wo_ref, lanes(cc * 2 + (m - 1) % 2, W), pl.ds(0, W))]

    inward = 1 - 2 * half

    def own_copies(m, k, cc):
        step = (inward, -inward)[k]
        return [remote(w.at[rows(dp, QR), cols], bufs[m].at[2 * z + c, rows(dp, QR), at], so.at[m, k, cc], zr.at[m, z, c], dp, (z + step) * 2 + cc)
                for w, cols, at in mine(m, cc)]

    def own_sends(ms, k):
        for m in ms:
            for cc in (0, 1):
                for cp in own_copies(m, k, cc):
                    cp.start()

    def zfwd(m, r, cc):
        o = origin(r)
        step = (1 if r == 1 else -1) * inward
        part = bufs[m].at[2 * o + cc, rows(dp, QR)]
        return remote(part, part, sf.at[m, r - 1, cc], zr.at[m, o, cc], dp, (z + step) * 2 + c)

    def zwait(m, r):
        for cc in (0, 1):
            zfwd(m, r, cc).wait_recv()

    def zforward(m, r):
        for cc in (0, 1):
            zfwd(m, r, cc).start()

    def plane(m, r, k):
        o, b = origin(r), bufs[m]
        part = (b.at[pl.ds(2 * o, 2), rows(dp, QR)], b.at[pl.ds(2 * o, 2), rows(dp, QR)], b.at[2 * o, rows(xd, QR)], b.at[2 * o + 1, rows(yd, QR)])[k]
        return remote(part, part, fs.at[m, r - 1, k], fr.at[m, r - 1, k], (xd, yd, yd, xd)[k], sp)

    def plane_in(m, r, k):
        o, b = origin(r), bufs[m]
        part = (b.at[pl.ds(2 * o, 2), rows(xd, QR)], b.at[pl.ds(2 * o, 2), rows(yd, QR)], b.at[2 * o, rows(diag, QR)], b.at[2 * o + 1, rows(diag, QR)])[k]
        return remote(part, part, fs.at[m, r - 1, k], fr.at[m, r - 1, k], (xd, yd, yd, xd)[k], sp)

    def xyforward(ms, r):
        for m in ms:
            plane(m, r, 0).start()
            plane(m, r, 1).start()

    def second(ms, r):
        for m in ms:
            plane_in(m, r, 0).wait_recv()
            plane_in(m, r, 1).wait_recv()
            plane(m, r, 2).start()
            plane(m, r, 3).start()

    def third(m, r):
        plane_in(m, r, 2).wait_recv()
        plane_in(m, r, 3).wait_recv()

    def relay(ms, r):
        for m in ms:
            zwait(m, r)
            zforward(m, r)

    def take(ms, r):
        for m in ms:
            zwait(m, r)
            xyforward((m,), r)

    def first(ms, r):
        for m in ms:
            zwait(m, r)
            pl.when(mid)(functools.partial(zforward, m, r))
            xyforward((m,), r)

    def shared(m):
        return [remote(w.at[:, cols], bufs[m].at[2 * z + c, :, at], ps.at[2 + m], pr.at[2 + m], dp, partner) for w, cols, at in mine(m, 1 - c)]

    def shared_wait(m):
        part = bufs[m].at[2 * z + 1 - c]
        remote(part, part, ps.at[2 + m], pr.at[2 + m], dp, partner).wait_recv()

    x_near = pltpu.make_async_copy(x_ref, xa.at[rows(c, H)], xl.at[0])
    x_far = remote(x_ref, xa.at[rows(c, H)], ps.at[0], pr.at[0], dp, partner)
    x_rest = remote(x_ref.at[:, lanes(1 - c, 2048)], xp_ref, ps.at[1], pr.at[1], dp, partner)

    def loads(m, r, slot):
        if r == 0:
            near = [pltpu.make_async_copy(w.at[:, cols], wst.at[slot, rows(c, H), at], ld.at[slot, i]) for i, (w, cols, at) in enumerate(mine(m, c))]
            return near + [pltpu.make_async_copy(bufs[m].at[2 * z + 1 - c], wst.at[slot, rows(1 - c, H), pl.ds(0, W)], ld.at[slot, 2])]
        o = origin(r)
        return [pltpu.make_async_copy(bufs[m].at[2 * o + i], wst.at[slot, pl.ds(i * H, H), pl.ds(0, W)], ld.at[slot, i]) for i in (0, 1)]

    def load(m, r, slot):
        for cp in loads(m, r, slot):
            cp.start()

    def loaded(m, r, slot):
        for cp in loads(m, r, slot):
            cp.wait()

    def part(r):
        return lanes(z if r == 0 else origin(r), T)

    def multiply(m, r, slot):
        depth = part(r)

        @pl.loop(0, W // 256)
        def _(i):
            cols, to = lanes(i, 256), lanes(i + (0 if m == 0 else (m - 1) % 2 * 4), 256)
            w = wst[slot, :, cols]
            for j in (0, 1):
                at = pl.ds(j * H, H)
                got = _dot(xa[at, depth], w, 1, 0)
                if r == 0:
                    acc[at, to] = got
                else:
                    acc[at, to] += got

    def project(ms, r):
        slots = (r % 2) * 2
        for i, m in enumerate(ms):
            load(m, r, slots + i)
        for i, m in enumerate(ms):
            loaded(m, r, slots + i)
            multiply(m, r, slots + i)

    def turned(t):
        t = t.astype(BF).astype(F32)
        return (t * cos_ref[...] + pltpu.roll(t, HEAD // 2, 1) * sin_ref[...]).astype(BF)

    def kv_out(d):
        o = z - d
        return [remote(b.at[o], b.at[o], cs.at[d, i], cr.at[d, i], dp, sp + 2) for i, b in enumerate((ks, vs))]

    def kv_in(d):
        o = z - d
        return [remote(b.at[o], b.at[o], cs.at[d - 1, i], cr.at[d - 1, i], dp, sp) for i, b in enumerate((ks, vs))]

    def kv_wait(d):
        for cp in kv_in(d):
            cp.wait_recv()

    def kv_send(d):
        for cp in kv_out(d):
            cp.start()

    def kv_pass(d):
        kv_wait(d)
        kv_send(d)

    e = HEAD**-0.5 * LOG2E

    def block(o, g, keys, strips, fresh):
        k = ks[o, g, keys, :]
        scores = [_dot(k, q_s[g, at : at + STRIP, :], 1, 1) for at, _ in strips]
        values = jnp.concatenate([vs[o, g, :, keys], jnp.ones((8, KB), BF)], axis=0)
        weights, keeps = [], []
        for (at, gap), s in zip(strips, scores):
            if gap is not None:
                ok = lax.broadcasted_iota(jnp.int32, (KB, STRIP), 1) + gap >= lax.broadcasted_iota(jnp.int32, (KB, STRIP), 0)
                s = jnp.where(ok, s, HIDDEN)
            top = s.max(axis=0, keepdims=True)
            if not fresh:
                old = top_s[g, :, at : at + STRIP]
                top = jnp.maximum(old, top)
                keeps.append(jnp.exp2((old - top) * e))
            top_s[g, :, at : at + STRIP] = top
            weights.append(jnp.exp2((s - top) * e).astype(BF))
        for i, ((at, _), p) in enumerate(zip(strips, weights)):
            got = _dot(values, p, 1, 0)
            if fresh:
                mix_s[g, :, at : at + STRIP] = got
            else:
                mix_s[g, :, at : at + STRIP] = mix_s[g, :, at : at + STRIP] * keeps[i] + got

    def attend_own():
        @pl.loop(0, 4)
        def _(g):
            block(z, g, pl.ds(0, KB), [(at, 0 if at % T == 0 else None) for at in range(0, 4 * T, STRIP)], True)
            block(z, g, pl.ds(KB, KB), [(at, 0) for at in range(STRIP, 4 * T, T)], False)

    def attend(d, lo=0, hi=8):
        @pl.loop(lo, hi)
        def _(i):
            block(z - d, i // 2, lanes(i % 2, KB), [(at, None) for at in range(0, 4 * T, STRIP)], False)

    def seen_copy(g):
        cols = lanes(c * 4 + g, 512)
        return remote(xa.at[:, cols], xa.at[:, cols], hs.at[g], hr.at[g], dp, partner)

    def seen_in(g):
        cols = lanes((1 - c) * 4 + g, 512)
        return remote(xa.at[:, cols], xa.at[:, cols], hs.at[g], hr.at[g], dp, partner)

    barrier = pltpu.get_barrier_semaphore()
    greeted = [(dp, partner), (xd, sp), (yd, sp)]
    for d, s in greeted:
        pl.semaphore_signal(barrier, inc=1, device_id={"dp": d, "sp": s}, device_id_type=MESH)
    for near, step in ((z >= 0, inward), (mid, -inward)):
        @pl.when(near)
        def _():
            for cc in (0, 1):
                pl.semaphore_signal(barrier, inc=1, device_id={"dp": dp, "sp": (z + step) * 2 + cc}, device_id_type=MESH)
    pl.semaphore_wait(barrier, len(greeted) + 2 + 2 * inner)

    end, last = inner == 0, z == 3

    def run(when, *steps):
        @pl.when(when)
        def _():
            for f, *args in steps:
                f(*args)

    own_sends(KV, 0)
    run(mid, (own_sends, KV, 1))
    run(end, (own_sends, Q, 0))
    x_near.start()
    x_far.start()
    for m in KV + Q:
        for cp in shared(m):
            cp.start()
    x_near.wait()
    x_far.wait_recv()

    def norm():
        @pl.loop(0, T // 32)
        def _(i):
            at = rows(i, 32)
            wide = xa[at, :].astype(F32)
            scale = lax.rsqrt(jnp.mean(wide * wide, -1, keepdims=True) + 1e-6)
            xa[at, :] = (wide * scale * gain_ref[...].astype(F32)).astype(BF)

    norm()
    first(KV, 1)
    run(mid, (own_sends, Q, 0))
    shared_wait(0)
    project(KV, 0)
    first(KV, 2)
    second(KV, 1)
    first(KV, 3)
    run(mid, (own_sends, Q, 1), (relay, Q, 1))
    second(KV, 2)
    run(mid, (relay, Q[:1], 2))
    second(KV, 3)
    run(mid, (xyforward, Q, 1), (relay, Q[1:], 2))
    third(0, 1)
    project(KV, 1)
    third(0, 2)
    project(KV, 2)
    run(end, (take, Q[:1], 1))
    third(0, 3)
    project(KV, 3)

    def make_kv():
        for g in range(4):
            ks[z, g] = turned(acc[:, g * HEAD : (g + 1) * HEAD])
            vs[z, g] = acc[:, 512 + g * HEAD : 512 + (g + 1) * HEAD].T.astype(BF)

    make_kv()
    run(mid, (relay, Q, 3))
    run(z < 3, (kv_send, 0))
    own_sends(O, 0)
    run(mid, (own_sends, O, 1))
    run(end, (take, Q[1:], 1))
    x_rest.start()
    for m in O:
        for cp in shared(m):
            cp.start()
    for m in Q:
        shared_wait(m)
    project(Q, 0)
    run(end, (take, Q, 2))
    run(mid, (xyforward, Q, 2))
    second(Q, 1)
    run(end, (take, Q, 3))
    run(mid, (xyforward, Q, 3))
    for m in Q:
        third(m, 1)
    project(Q, 1)
    second(Q, 2)
    run(mid, (kv_pass, 1))
    second(Q, 3)
    for m in Q:
        third(m, 2)
    project(Q, 2)
    run(z < 3, (first, O, 1))
    for m in Q:
        third(m, 3)
    project(Q, 3)
    pl.semaphore_signal(rdy, inc=1, device_id={"dp": dp, "sp": partner}, device_id_type=MESH)

    def make_q():
        @pl.loop(0, 4)
        def _(g):
            for n in range(4):
                q_s[g, n * T : (n + 1) * T, :] = turned(acc[:, lanes(g * 4 + n, HEAD)])

    make_q()
    run(last, (take, O, 1))
    attend_own()
    run(z < 3, (first, O, 2))
    run(z == 2, (kv_pass, 2))
    second(O, 1)
    run(last, (kv_wait, 1))
    run(z >= 1, (attend, 1))
    run(z < 3, (first, O, 3))
    run(last, (kv_wait, 2))
    run(z >= 2, (attend, 2))
    run(last, (take, O, 2))
    second(O, 2)
    run(last, (kv_wait, 3), (attend, 3, 0, 4), (take, O[:1], 3), (attend, 3, 4, 8))

    def finish():
        pl.semaphore_wait(rdy, 1)

        @pl.loop(0, 4)
        def _(g):
            for n in range(4):
                at = slice(n * T, (n + 1) * T)
                out = mix_s[g, :HEAD, at] * (1 / mix_s[g, HEAD : HEAD + 1, at])
                xa[:, lanes(c * 16 + g * 4 + n, HEAD)] = out.T.astype(BF)
            seen_copy(g).start()

    finish()
    run(last, (take, O[1:], 3))
    for m in O:
        shared_wait(m)
        load(m, 0, m - 3)
    for m in O:
        third(m, 1)
        load(m, 1, m - 1)

    def seen_wait():
        for g in range(4):
            seen_in(g).wait_recv()

    seen_wait()

    def times(r, slot):
        for m in O:
            loaded(m, r, slot + m - 3)
            multiply(m, r, slot + m - 3)

    times(0, 0)
    second(O[:1], 3)
    for m in O:
        third(m, 2)
        load(m, 2, m - 3)
    times(1, 2)
    x_rest.wait_recv()
    rest_x = [cp for h in (0, 1) for cp in (
        pltpu.make_async_copy(x_ref.at[:, lanes(c * 2 + h, W)], wst.at[2 + h, rows(c, H)], xl.at[1 + h]),
        pltpu.make_async_copy(xp_ref.at[:, pl.ds(h * W, W)], wst.at[2 + h, rows(1 - c, H)], xl.at[3 + h]))]
    for cp in rest_x:
        cp.start()
    second(O[1:], 3)
    times(2, 0)
    for cp in rest_x:
        cp.wait()

    def results(i):
        cols, to = pl.ds(i % 2 * 512, 512), lanes(c * 4 + i, 512)
        return (pltpu.make_async_copy(wst.at[2 + i // 2, rows(c, H), cols], y_ref.at[:, to], xl.at[5 + i]),
                remote(wst.at[2 + i // 2, rows(1 - c, H), cols], y_ref.at[:, to], ys.at[i], yr.at[i], dp, partner))

    def result_in(i):
        to = lanes((1 - c) * 4 + i, 512)
        return remote(y_ref.at[:, to], y_ref.at[:, to], ys.at[i], yr.at[i], dp, partner)

    def final(h):
        depth, m = part(3), O[h]
        third(m, 3)
        load(m, 3, h)
        loaded(m, 3, h)
        for i in (0, 1):
            for n in (0, 1):
                cols = slice(i * 512 + n * 256, i * 512 + n * 256 + 256)
                for j in (0, 1):
                    at = slice(j * H, (j + 1) * H)
                    got = acc[at, h * W + cols.start : h * W + cols.stop] + _dot(xa[at, depth], wst[h, :, cols], 1, 0)
                    wst[2 + h, at, cols] = (wst[2 + h, at, cols].astype(F32) + got).astype(BF)
            for cp in results(2 * h + i):
                cp.start()

    final(0)
    final(1)

    for i in range(4):
        near, far = results(i)
        near.wait()
        far.wait_send()
        result_in(i).wait_recv()
        seen_copy(i).wait_send()
    x_far.wait_send()
    x_rest.wait_send()
    for m in KV + Q + O:
        here = bufs[m].at[2 * z + c]
        remote(here, here, ps.at[2 + m], pr.at[2 + m], dp, partner).wait_send()
        quarter = bufs[m].at[2 * z + c, rows(dp, QR)]
        for k in (0, 1):
            @pl.when(mid | (k == 0))
            def _():
                for cc in (0, 1):
                    remote(quarter, quarter, so.at[m, k, cc], zr.at[m, z, c], dp, (z + (inward, -inward)[k]) * 2 + cc).wait_send()
        for r in (1, 2, 3):
            @pl.when(mid)
            def _():
                for cc in (0, 1):
                    zfwd(m, r, cc).wait_send()
            for k in range(4):
                plane(m, r, k).wait_send()
    for d in (0, 1, 2):
        @pl.when((z >= d) & (z < 3))
        def _():
            for cp in kv_out(d):
                cp.wait_send()


def solution(mesh):
    def step(x, gain, wq, wk, wv, wo):
        place = (lax.axis_index("sp") // 2) * T + jnp.arange(T)
        angle = place.astype(F32)[:, None] * THETA ** (-jnp.arange(HEAD // 2, dtype=F32) / (HEAD // 2))
        cos, sin = jnp.cos(angle), jnp.sin(angle)
        cos, sin = jnp.concatenate([cos, cos], 1), jnp.concatenate([-sin, sin], 1)
        far, near = pl.BlockSpec(memory_space=pl.ANY), pl.BlockSpec(memory_space=pltpu.VMEM)
        sems = pltpu.SemaphoreType.DMA
        y, *_ = pl.pallas_call(
            _layer,
            out_shape=[
                jax.ShapeDtypeStruct((H, D), BF),
                jax.ShapeDtypeStruct((H, 2048), BF),
                *[jax.ShapeDtypeStruct((8, H, W), BF)] * 5,
            ],
            in_specs=[far, near, far, far, far, far, near, near],
            out_specs=[far] * 7,
            scratch_shapes=[
                pltpu.VMEM((T, D), BF),
                pltpu.VMEM((4, T, W), BF),
                pltpu.VMEM((T, 2048), F32),
                pltpu.VMEM((4, 4 * T, HEAD), BF),
                pltpu.VMEM((4, 4, T, HEAD), BF),
                pltpu.VMEM((4, 4, HEAD, T), BF),
                pltpu.VMEM((4, HEAD + 8, 4 * T), F32),
                pltpu.VMEM((4, 1, 4 * T), F32),
                sems((5, 2, 2)),
                sems((5, 3, 2)),
                sems((5, 4, 2)),
                sems((5, 3, 4)),
                sems((5, 3, 4)),
                sems((3, 2)),
                sems((3, 2)),
                sems((7,)),
                sems((7,)),
                sems((4,)),
                sems((4,)),
                sems((4,)),
                sems((4,)),
                sems((4, 3)),
                sems((9,)),
                pltpu.SemaphoreType.REGULAR,
            ],
            compiler_params=pltpu.CompilerParams(collective_id=0, has_side_effects=True, vmem_limit_bytes=63 * 2**20),
        )(x, gain[None], wq, wk, wv, wo, cos, sin)
        return y

    tokens, whole = P(("dp", "sp"), None), P("sp", None)
    return jax.shard_map(
        step,
        mesh=mesh,
        in_specs=(tokens, P(None), whole, whole, whole, whole),
        out_specs=tokens,
        check_vma=False,
    )
```

```python
import functools

import jax
import jax.numpy as jnp
from jax import lax
from jax.experimental import pallas as pl
from jax.experimental.pallas import tpu as pltpu
from jax.sharding import PartitionSpec as P

HEAD = 128
THETA = 10000
NEG = -1e30
HIDDEN = 2 * NEG
LOG2E = 1.4426950408889634
MESH = pl.DeviceIdType.MESH
BF = jnp.bfloat16
F32 = jnp.float32

T = 1024
D = 4096
H = 512
QR = 128
W = 1024
KV, Q, O = (0,), (1, 2), (3, 4)
KB = 512
STRIP = 512


def _dot(a, b, ca, cb):
    return lax.dot_general(a, b, (((ca,), (cb,)), ((), ())), preferred_element_type=F32)


def _layer(x_ref, gain_ref, wq_ref, wk_ref, wv_ref, wo_ref, freq_ref, y_ref, xp_ref, b0, b1, b2, b3, b4, xa, wst, acc, q_s, ks, vs, mix_s,
           top_s, cos_ref, sin_ref, so, sf, zr, fs, fr, cs, cr, ps, pr, hs, hr, ys, yr, ld, xl, rdy):
    dp, sp = lax.axis_index("dp"), lax.axis_index("sp")
    z, c = sp // 2, sp % 2
    jx, jy = dp // 2, dp % 2
    xd, yd, diag = (1 - jx) * 2 + jy, jx * 2 + 1 - jy, 3 - dp
    half = z // 2
    inner = z + half * (3 - 2 * z)
    mid = inner == 1
    partner = z * 2 + 1 - c
    bufs = (b0, b1, b2, b3, b4)

    def remote(src, dst, send, recv, d, s):
        return pltpu.make_async_remote_copy(src_ref=src, dst_ref=dst, send_sem=send, recv_sem=recv, device_id={"dp": d, "sp": s}, device_id_type=MESH)

    def lanes(i, n):
        return pl.ds(pl.multiple_of(i * n, n), n)

    def rows(i, n):
        return pl.ds(pl.multiple_of(i * n, n), n)

    def origin(r):
        base = (1 - inner, 2, 3)[r - 1]
        return base + half * (3 - 2 * base)

    def mine(m, cc):
        if m == 0:
            return [(wk_ref, lanes(cc, 512), pl.ds(0, 512)), (wv_ref, lanes(cc, 512), pl.ds(512, 512))]
        return [(wq_ref if m in Q else wo_ref, lanes(cc * 2 + (m - 1) % 2, W), pl.ds(0, W))]

    inward = 1 - 2 * half

    def own_copies(m, k, cc):
        step = (inward, -inward)[k]
        return [remote(w.at[rows(dp, QR), cols], bufs[m].at[2 * z + c, rows(dp, QR), at], so.at[m, k, cc], zr.at[m, z, c], dp, (z + step) * 2 + cc)
                for w, cols, at in mine(m, cc)]

    def own_sends(ms, k):
        for m in ms:
            for cc in (0, 1):
                for cp in own_copies(m, k, cc):
                    cp.start()

    def zfwd(m, r, cc):
        o = origin(r)
        step = (1 if r == 1 else -1) * inward
        part = bufs[m].at[2 * o + cc, rows(dp, QR)]
        return remote(part, part, sf.at[m, r - 1, cc], zr.at[m, o, cc], dp, (z + step) * 2 + c)

    def zwait(m, r):
        for cc in (0, 1):
            zfwd(m, r, cc).wait_recv()

    def zforward(m, r):
        for cc in (0, 1):
            zfwd(m, r, cc).start()

    def plane(m, r, k):
        o, b = origin(r), bufs[m]
        part = (b.at[pl.ds(2 * o, 2), rows(dp, QR)], b.at[pl.ds(2 * o, 2), rows(dp, QR)], b.at[2 * o, rows(xd, QR)], b.at[2 * o + 1, rows(yd, QR)])[k]
        return remote(part, part, fs.at[m, r - 1, k], fr.at[m, r - 1, k], (xd, yd, yd, xd)[k], sp)

    def plane_in(m, r, k):
        o, b = origin(r), bufs[m]
        part = (b.at[pl.ds(2 * o, 2), rows(xd, QR)], b.at[pl.ds(2 * o, 2), rows(yd, QR)], b.at[2 * o, rows(diag, QR)], b.at[2 * o + 1, rows(diag, QR)])[k]
        return remote(part, part, fs.at[m, r - 1, k], fr.at[m, r - 1, k], (xd, yd, yd, xd)[k], sp)

    def xyforward(ms, r):
        for m in ms:
            plane(m, r, 0).start()
            plane(m, r, 1).start()

    def second(ms, r):
        for m in ms:
            plane_in(m, r, 0).wait_recv()
            plane_in(m, r, 1).wait_recv()
            plane(m, r, 2).start()
            plane(m, r, 3).start()

    def third(m, r):
        plane_in(m, r, 2).wait_recv()
        plane_in(m, r, 3).wait_recv()

    def relay(ms, r):
        for m in ms:
            zwait(m, r)
            zforward(m, r)

    def take(ms, r):
        for m in ms:
            zwait(m, r)
            xyforward((m,), r)

    def first(ms, r):
        for m in ms:
            zwait(m, r)
            pl.when(mid)(functools.partial(zforward, m, r))
            xyforward((m,), r)

    def shared(m):
        return [remote(w.at[:, cols], bufs[m].at[2 * z + c, :, at], ps.at[2 + m], pr.at[2 + m], dp, partner) for w, cols, at in mine(m, 1 - c)]

    def shared_wait(m):
        part = bufs[m].at[2 * z + 1 - c]
        remote(part, part, ps.at[2 + m], pr.at[2 + m], dp, partner).wait_recv()

    x_near = pltpu.make_async_copy(x_ref, xa.at[rows(c, H)], xl.at[0])
    x_far = remote(x_ref, xa.at[rows(c, H)], ps.at[0], pr.at[0], dp, partner)
    x_rest = remote(x_ref.at[:, lanes(1 - c, 2048)], xp_ref, ps.at[1], pr.at[1], dp, partner)

    def loads(m, r, slot):
        if r == 0:
            near = [pltpu.make_async_copy(w.at[:, cols], wst.at[slot, rows(c, H), at], ld.at[slot, i]) for i, (w, cols, at) in enumerate(mine(m, c))]
            return near + [pltpu.make_async_copy(bufs[m].at[2 * z + 1 - c], wst.at[slot, rows(1 - c, H), pl.ds(0, W)], ld.at[slot, 2])]
        o = origin(r)
        return [pltpu.make_async_copy(bufs[m].at[2 * o + i], wst.at[slot, pl.ds(i * H, H), pl.ds(0, W)], ld.at[slot, i]) for i in (0, 1)]

    def load(m, r, slot):
        for cp in loads(m, r, slot):
            cp.start()

    def loaded(m, r, slot):
        for cp in loads(m, r, slot):
            cp.wait()

    def part(r):
        return lanes(z if r == 0 else origin(r), T)

    def multiply(m, r, slot):
        depth = part(r)

        @pl.loop(0, W // 256)
        def _(i):
            cols, to = lanes(i, 256), lanes(i + (0 if m == 0 else (m - 1) % 2 * 4), 256)
            w = wst[slot, :, cols]
            for j in (0, 1):
                at = pl.ds(j * H, H)
                got = _dot(xa[at, depth], w, 1, 0)
                if r == 0:
                    acc[at, to] = got
                else:
                    acc[at, to] += got

    def project(ms, r):
        slots = (r % 2) * 2
        for i, m in enumerate(ms):
            load(m, r, slots + i)
        for i, m in enumerate(ms):
            loaded(m, r, slots + i)
            multiply(m, r, slots + i)

    def turned(t):
        t = t.astype(BF).astype(F32)
        return (t * cos_ref[...] + pltpu.roll(t, HEAD // 2, 1) * sin_ref[...]).astype(BF)

    def kv_out(d):
        o = z - d
        return [remote(b.at[o], b.at[o], cs.at[d, i], cr.at[d, i], dp, sp + 2) for i, b in enumerate((ks, vs))]

    def kv_in(d):
        o = z - d
        return [remote(b.at[o], b.at[o], cs.at[d - 1, i], cr.at[d - 1, i], dp, sp) for i, b in enumerate((ks, vs))]

    def kv_wait(d):
        for cp in kv_in(d):
            cp.wait_recv()

    def kv_send(d):
        for cp in kv_out(d):
            cp.start()

    def kv_pass(d):
        kv_wait(d)
        kv_send(d)

    e = HEAD**-0.5 * LOG2E

    def block(o, g, keys, strips, fresh):
        k = ks[o, g, keys, :]
        scores = [_dot(k, q_s[g, at : at + STRIP, :], 1, 1) for at, _ in strips]
        values = jnp.concatenate([vs[o, g, :, keys], jnp.ones((8, KB), BF)], axis=0)
        weights, keeps = [], []
        for (at, gap), s in zip(strips, scores):
            if gap is not None:
                ok = lax.broadcasted_iota(jnp.int32, (KB, STRIP), 1) + gap >= lax.broadcasted_iota(jnp.int32, (KB, STRIP), 0)
                s = jnp.where(ok, s, HIDDEN)
            top = s.max(axis=0, keepdims=True)
            if not fresh:
                old = top_s[g, :, at : at + STRIP]
                top = jnp.maximum(old, top)
                keeps.append(jnp.exp2((old - top) * e))
            top_s[g, :, at : at + STRIP] = top
            weights.append(jnp.exp2((s - top) * e).astype(BF))
        for i, ((at, _), p) in enumerate(zip(strips, weights)):
            got = _dot(values, p, 1, 0)
            if fresh:
                mix_s[g, :, at : at + STRIP] = got
            else:
                mix_s[g, :, at : at + STRIP] = mix_s[g, :, at : at + STRIP] * keeps[i] + got

    def attend_own():
        @pl.loop(0, 4)
        def _(g):
            block(z, g, pl.ds(0, KB), [(at, 0 if at % T == 0 else None) for at in range(0, 4 * T, STRIP)], True)
            block(z, g, pl.ds(KB, KB), [(at, 0) for at in range(STRIP, 4 * T, T)], False)

    def attend(d):
        @pl.loop(0, 8)
        def _(i):
            block(z - d, i // 2, lanes(i % 2, KB), [(at, None) for at in range(0, 4 * T, STRIP)], False)

    def seen_copy(g):
        cols = lanes(c * 4 + g, 512)
        return remote(xa.at[:, cols], xa.at[:, cols], hs.at[g], hr.at[g], dp, partner)

    def seen_in(g):
        cols = lanes((1 - c) * 4 + g, 512)
        return remote(xa.at[:, cols], xa.at[:, cols], hs.at[g], hr.at[g], dp, partner)

    barrier = pltpu.get_barrier_semaphore()
    greeted = [(dp, partner), (xd, sp), (yd, sp)]
    for d, s in greeted:
        pl.semaphore_signal(barrier, inc=1, device_id={"dp": d, "sp": s}, device_id_type=MESH)
    for near, step in ((z >= 0, inward), (mid, -inward)):
        @pl.when(near)
        def _():
            for cc in (0, 1):
                pl.semaphore_signal(barrier, inc=1, device_id={"dp": dp, "sp": (z + step) * 2 + cc}, device_id_type=MESH)
    pl.semaphore_wait(barrier, len(greeted) + 2 + 2 * inner)

    end, last = inner == 0, z == 3

    def run(when, *steps):
        @pl.when(when)
        def _():
            for f, *args in steps:
                f(*args)

    own_sends(KV, 0)
    run(mid, (own_sends, KV, 1))
    run(end, (own_sends, Q, 0))
    x_near.start()
    x_far.start()
    for m in KV + Q:
        for cp in shared(m):
            cp.start()
    x_near.wait()
    x_far.wait_recv()

    def norm():
        @pl.loop(0, T // 32)
        def _(i):
            at = rows(i, 32)
            wide = xa[at, :].astype(F32)
            scale = lax.rsqrt(jnp.mean(wide * wide, -1, keepdims=True) + 1e-6)
            xa[at, :] = (wide * scale * gain_ref[...].astype(F32)[None]).astype(BF)

    norm()
    first(KV, 1)
    run(mid, (own_sends, Q, 0))
    shared_wait(0)
    project(KV, 0)

    def tables():
        @pl.loop(0, 8)
        def _(i):
            at = rows(i, 128)
            place = z * T + i * 128 + lax.broadcasted_iota(jnp.int32, (128, HEAD), 0)
            angle = place.astype(F32) * freq_ref[...][None]
            cos_ref[at, :] = jnp.cos(angle)
            sin_ref[at, :] = jnp.sin(angle) * jnp.where(lax.broadcasted_iota(jnp.int32, (128, HEAD), 1) < HEAD // 2, -1.0, 1.0)

    tables()
    first(KV, 2)
    second(KV, 1)
    first(KV, 3)
    run(mid, (own_sends, Q, 1), (relay, Q, 1))
    second(KV, 2)
    run(mid, (relay, Q[:1], 2))
    second(KV, 3)
    run(mid, (xyforward, Q, 1), (relay, Q[1:], 2))
    third(0, 1)
    project(KV, 1)
    third(0, 2)
    project(KV, 2)
    run(end, (take, Q[:1], 1))
    third(0, 3)
    project(KV, 3)

    def make_kv():
        for g in range(4):
            ks[z, g] = turned(acc[:, g * HEAD : (g + 1) * HEAD])
            vs[z, g] = acc[:, 512 + g * HEAD : 512 + (g + 1) * HEAD].T.astype(BF)

    make_kv()
    run(mid, (relay, Q, 3))
    run(z < 3, (kv_send, 0))
    own_sends(O, 0)
    run(mid, (own_sends, O, 1))
    run(end, (take, Q[1:], 1))
    x_rest.start()
    for m in O:
        for cp in shared(m):
            cp.start()
    for m in Q:
        shared_wait(m)
    project(Q, 0)
    run(end, (take, Q, 2))
    run(mid, (xyforward, Q, 2))
    second(Q, 1)
    run(end, (take, Q, 3))
    run(mid, (xyforward, Q, 3))
    for m in Q:
        third(m, 1)
    project(Q, 1)
    second(Q, 2)
    run(mid, (kv_pass, 1))
    second(Q, 3)
    for m in Q:
        third(m, 2)
    project(Q, 2)
    run(z < 3, (first, O, 1))
    for m in Q:
        third(m, 3)
    project(Q, 3)
    pl.semaphore_signal(rdy, inc=1, device_id={"dp": dp, "sp": partner}, device_id_type=MESH)

    def make_q():
        @pl.loop(0, 4)
        def _(g):
            for n in range(4):
                q_s[g, n * T : (n + 1) * T, :] = turned(acc[:, lanes(g * 4 + n, HEAD)])

    make_q()
    run(last, (take, O, 1))
    attend_own()
    run(z < 3, (first, O, 2))
    run(z == 2, (kv_pass, 2))
    second(O, 1)
    run(last, (kv_wait, 1))
    run(z >= 1, (attend, 1))
    run(z < 3, (first, O, 3))
    run(last, (kv_wait, 2))
    run(z >= 2, (attend, 2))
    run(last, (take, O, 2))
    second(O, 2)
    pl.semaphore_wait(rdy, 1)

    def finish(g):
        for n in range(4):
            at = slice(n * T, (n + 1) * T)
            out = mix_s[g, :HEAD, at] * (1 / mix_s[g, HEAD : HEAD + 1, at])
            xa[:, lanes(c * 16 + g * 4 + n, HEAD)] = out.T.astype(BF)
        seen_copy(g).start()

    def attend_last():
        kv_wait(3)

        @pl.loop(0, 4)
        def _(g):
            @pl.loop(0, 2)
            def _(i):
                block(z - 3, g, lanes(i, KB), [(at, None) for at in range(0, 4 * T, STRIP)], False)

            finish(g)
            run(g == 1, (take, O[:1], 3))

        take(O[1:], 3)

    def finish_all():
        pl.loop(0, 4)(finish)

    run(last, (attend_last,))
    run(z < 3, (finish_all,))

    for m in O:
        shared_wait(m)
        load(m, 0, m - 3)
    for m in O:
        third(m, 1)
        load(m, 1, m - 1)

    def seen_wait():
        for g in range(4):
            seen_in(g).wait_recv()

    seen_wait()

    def times(r, slot):
        for m in O:
            loaded(m, r, slot + m - 3)
            multiply(m, r, slot + m - 3)

    times(0, 0)
    second(O[:1], 3)
    for m in O:
        third(m, 2)
        load(m, 2, m - 3)
    times(1, 2)
    x_rest.wait_recv()
    rest_x = [cp for h in (0, 1) for cp in (
        pltpu.make_async_copy(x_ref.at[:, lanes(c * 2 + h, W)], wst.at[2 + h, rows(c, H)], xl.at[1 + h]),
        pltpu.make_async_copy(xp_ref.at[:, pl.ds(h * W, W)], wst.at[2 + h, rows(1 - c, H)], xl.at[3 + h]))]
    for cp in rest_x:
        cp.start()
    second(O[1:], 3)
    times(2, 0)
    for cp in rest_x:
        cp.wait()

    def results(i):
        cols, to = pl.ds(i % 2 * 512, 512), lanes(c * 4 + i, 512)
        return (pltpu.make_async_copy(wst.at[2 + i // 2, rows(c, H), cols], y_ref.at[:, to], xl.at[5 + i]),
                remote(wst.at[2 + i // 2, rows(1 - c, H), cols], y_ref.at[:, to], ys.at[i], yr.at[i], dp, partner))

    def result_in(i):
        to = lanes((1 - c) * 4 + i, 512)
        return remote(y_ref.at[:, to], y_ref.at[:, to], ys.at[i], yr.at[i], dp, partner)

    def final(h):
        depth, m = part(3), O[h]
        third(m, 3)
        load(m, 3, h)
        loaded(m, 3, h)
        for i in (0, 1):
            for n in (0, 1):
                cols = slice(i * 512 + n * 256, i * 512 + n * 256 + 256)
                for j in (0, 1):
                    at = slice(j * H, (j + 1) * H)
                    got = acc[at, h * W + cols.start : h * W + cols.stop] + _dot(xa[at, depth], wst[h, :, cols], 1, 0)
                    wst[2 + h, at, cols] = (wst[2 + h, at, cols].astype(F32) + got).astype(BF)
            for cp in results(2 * h + i):
                cp.start()

    final(0)
    final(1)

    for i in range(4):
        near, far = results(i)
        near.wait()
        far.wait_send()
        result_in(i).wait_recv()
        seen_copy(i).wait_send()
    x_far.wait_send()
    x_rest.wait_send()
    for m in KV + Q + O:
        here = bufs[m].at[2 * z + c]
        remote(here, here, ps.at[2 + m], pr.at[2 + m], dp, partner).wait_send()
        quarter = bufs[m].at[2 * z + c, rows(dp, QR)]
        for k in (0, 1):
            @pl.when(mid | (k == 0))
            def _():
                for cc in (0, 1):
                    remote(quarter, quarter, so.at[m, k, cc], zr.at[m, z, c], dp, (z + (inward, -inward)[k]) * 2 + cc).wait_send()
        for r in (1, 2, 3):
            @pl.when(mid)
            def _():
                for cc in (0, 1):
                    zfwd(m, r, cc).wait_send()
            for k in range(4):
                plane(m, r, k).wait_send()
    for d in (0, 1, 2):
        @pl.when((z >= d) & (z < 3))
        def _():
            for cp in kv_out(d):
                cp.wait_send()


def solution(mesh):
    def step(x, gain, wq, wk, wv, wo):
        freq = THETA ** (-(jnp.arange(HEAD) % (HEAD // 2)).astype(F32) / (HEAD // 2))
        far, near = pl.BlockSpec(memory_space=pl.ANY), pl.BlockSpec(memory_space=pltpu.VMEM)
        sems = pltpu.SemaphoreType.DMA
        y, *_ = pl.pallas_call(
            _layer,
            out_shape=[
                jax.ShapeDtypeStruct((H, D), BF),
                jax.ShapeDtypeStruct((H, 2048), BF),
                *[jax.ShapeDtypeStruct((8, H, W), BF)] * 5,
            ],
            in_specs=[far, near, far, far, far, far, near],
            out_specs=[far] * 7,
            scratch_shapes=[
                pltpu.VMEM((T, D), BF),
                pltpu.VMEM((4, T, W), BF),
                pltpu.VMEM((T, 2048), F32),
                pltpu.VMEM((4, 4 * T, HEAD), BF),
                pltpu.VMEM((4, 4, T, HEAD), BF),
                pltpu.VMEM((4, 4, HEAD, T), BF),
                pltpu.VMEM((4, HEAD + 8, 4 * T), F32),
                pltpu.VMEM((4, 1, 4 * T), F32),
                pltpu.VMEM((T, HEAD), F32),
                pltpu.VMEM((T, HEAD), F32),
                sems((5, 2, 2)),
                sems((5, 3, 2)),
                sems((5, 4, 2)),
                sems((5, 3, 4)),
                sems((5, 3, 4)),
                sems((3, 2)),
                sems((3, 2)),
                sems((7,)),
                sems((7,)),
                sems((4,)),
                sems((4,)),
                sems((4,)),
                sems((4,)),
                sems((4, 3)),
                sems((9,)),
                pltpu.SemaphoreType.REGULAR,
            ],
            compiler_params=pltpu.CompilerParams(collective_id=0, has_side_effects=True, vmem_limit_bytes=63 * 2**20),
        )(x, gain, wq, wk, wv, wo, freq)
        return y

    tokens, whole = P(("dp", "sp"), None), P("sp", None)
    return jax.shard_map(
        step,
        mesh=mesh,
        in_specs=(tokens, P(None), whole, whole, whole, whole),
        out_specs=tokens,
        check_vma=False,
    )
```

```python
import functools

import jax
import jax.numpy as jnp
from jax import lax
from jax.experimental import pallas as pl
from jax.experimental.pallas import tpu as pltpu
from jax.sharding import PartitionSpec as P

HEAD = 128
THETA = 10000
NEG = -1e30
HIDDEN = 2 * NEG
LOG2E = 1.4426950408889634
MESH = pl.DeviceIdType.MESH
TWO, ROUNDS, FOUR = (0, 1), (1, 2, 3), range(4)
BF = jnp.bfloat16
F32 = jnp.float32

T = 1024
D = 4096
H = 512
QR = 128
W = 1024
KV, Q, O = (0, 1), (2, 3, 4), (5, 6)
OA, OB, QA, QB = O[:1], O[1:], Q[:1], Q[1:]
WID = (768, 256, 1024, 512, 512, 1024, 1024)
SHIP = (1, 4)
ACC = (0, 768, 0, 1024, 1536, 0, 1024)
SLOT = (0, 0, 0, 1, 1, 0, 1)
COL = (0, 768, 0, 0, 512, 0, 0)
KB = 512
STRIP = 512
QS = 4 * T
HALF = HEAD // 2
C = 2048


def _dot(a, b, cb=0):
    return lax.dot_general(a, b, (((1,), (cb,)), ((), ())), preferred_element_type=F32)


def _layer(x_ref, gain_ref, wq_ref, wk_ref, wv_ref, wo_ref, freq_ref, y_ref, xp_ref, a3, b0, b1, b2, b3, b4, b5, b6, xa, wst, acc, eacc, q_s, ks, vs, mix_s,
           top_s, cos_ref, sin_ref, so, sf, zr, fs, fr, cs, cr, ps, pr, hs, hr, ys, yr, ld, xl, hs3, hr3, es, er, rdy, rdy3):
    dp, sp = lax.axis_index("dp"), lax.axis_index("sp")
    z, c = sp // 2, sp % 2
    jx, jy = dp // 2, dp % 2
    xd, yd, diag = (1 - jx) * 2 + jy, jx * 2 + 1 - jy, 3 - dp
    half = z // 2
    inner = z + half * (3 - 2 * z)
    mid = inner == 1
    partner = z * 2 + 1 - c
    bufs = (b0, b1, b2, b3, b4, b5, b6)
    end, last, low, is1, is2 = inner == 0, z == 3, z < 3, z == 1, z == 2
    oc = 1 - c

    def run(when, *steps):
        @pl.when(when)
        def _():
            for f, *args in steps:
                f(*args)

    def each(f, ms, *args):
        for m in ms:
            if m in SHIP:
                run(low, (f, m, *args))
            else:
                f(m, *args)

    def upward(f, m, *args):
        if m in SHIP:
            run(z != 2, (f, m, *args))
        else:
            f(m, *args)

    def remote(src, dst, send, recv, d, s):
        return pltpu.make_async_remote_copy(src_ref=src, dst_ref=dst, send_sem=send, recv_sem=recv, device_id={"dp": d, "sp": s}, device_id_type=MESH)

    def lanes(i, n):
        return pl.ds(pl.multiple_of(i * n, n), n)

    def rows(i, n):
        return pl.ds(pl.multiple_of(i * n, n), n)

    def origin(r):
        base = (1 - inner, 2, 3)[r - 1]
        return base + half * (3 - 2 * base)

    def mine(m, cc):
        if m in KV:
            n, at = (384, 128)[m], cc * 512 + (0, 384)[m]
            cols = pl.ds(pl.multiple_of(at, 128), n)
            return [(wk_ref, cols, pl.ds(0, n)), (wv_ref, cols, pl.ds(n, n))]
        cols = pl.ds(pl.multiple_of(cc * C + ACC[m], 512), WID[m])
        return [(wq_ref if m in Q else wo_ref, cols, pl.ds(0, WID[m]))]

    inward = 1 - 2 * half

    def own_copies(m, k, cc):
        step = (inward, -inward)[k]
        return [remote(w.at[rows(dp, QR), cols], bufs[m].at[sp, rows(dp, QR), at], so.at[m, k, cc], zr.at[m, z, c], dp, (z + step) * 2 + cc)
                for w, cols, at in mine(m, cc)]

    def own_send(m, k):
        for cc in TWO:
            for cp in own_copies(m, k, cc):
                cp.start()

    def own_sends(ms, k):
        for m in ms:
            if k:
                upward(own_send, m, k)
            else:
                own_send(m, k)

    def zfwd(m, r, cc):
        o = origin(r)
        step = (1 if r == 1 else -1) * inward
        part = bufs[m].at[2 * o + cc, rows(dp, QR)]
        return remote(part, part, sf.at[m, r - 1, cc], zr.at[m, o, cc], dp, (z + step) * 2 + c)

    def zwait(m, r):
        for cc in TWO:
            zfwd(m, r, cc).wait_recv()

    def zforward_now(m, r):
        for cc in TWO:
            zfwd(m, r, cc).start()

    def zforward(m, r):
        if r == 1:
            zforward_now(m, r)
        else:
            upward(zforward_now, m, r)

    def plane(m, r, k):
        o, b = origin(r), bufs[m]
        part = (b.at[pl.ds(2 * o, 2), rows(dp, QR)], b.at[pl.ds(2 * o, 2), rows(dp, QR)], b.at[2 * o, rows(xd, QR)], b.at[2 * o + 1, rows(yd, QR)])[k]
        return remote(part, part, fs.at[m, r - 1, k], fr.at[m, r - 1, k], (xd, yd, yd, xd)[k], sp)

    def plane_in(m, r, k):
        o, b = origin(r), bufs[m]
        part = (b.at[pl.ds(2 * o, 2), rows(xd, QR)], b.at[pl.ds(2 * o, 2), rows(yd, QR)], b.at[2 * o, rows(diag, QR)], b.at[2 * o + 1, rows(diag, QR)])[k]
        return remote(part, part, fs.at[m, r - 1, k], fr.at[m, r - 1, k], (xd, yd, yd, xd)[k], sp)

    def spread(m, r):
        plane(m, r, 0).start()
        plane(m, r, 1).start()

    def xyforward(ms, r):
        each(spread, ms, r)

    def second_one(m, r):
        plane_in(m, r, 0).wait_recv()
        plane_in(m, r, 1).wait_recv()
        plane(m, r, 2).start()
        plane(m, r, 3).start()

    def second(ms, r):
        each(second_one, ms, r)

    def third_one(m, r):
        plane_in(m, r, 2).wait_recv()
        plane_in(m, r, 3).wait_recv()

    def third(ms, r):
        each(third_one, ms, r)

    def relay(ms, r):
        for m in ms:
            zwait(m, r)
            zforward(m, r)

    def take(ms, r):
        def one(m):
            zwait(m, r)
            spread(m, r)

        each(one, ms)

    def first(ms, r):
        def one(m):
            zwait(m, r)
            run(mid, (zforward, m, r))
            spread(m, r)

        each(one, ms)

    def shared(m):
        return [remote(w.at[:, cols], bufs[m].at[sp, :, at], ps.at[2 + m], pr.at[2 + m], dp, partner) for w, cols, at in mine(m, oc)]

    def share(m):
        for cp in shared(m):
            cp.start()

    def shared_wait(m):
        part = bufs[m].at[partner]
        remote(part, part, ps.at[2 + m], pr.at[2 + m], dp, partner).wait_recv()

    x_near = pltpu.make_async_copy(x_ref, xa.at[rows(c, H)], xl.at[0])
    x_far = remote(x_ref, xa.at[rows(c, H)], ps.at[0], pr.at[0], dp, partner)
    x_rest = remote(x_ref.at[:, lanes(oc, C)], xp_ref, ps.at[1], pr.at[1], dp, partner)

    def loads(m, r, pair, at=None):
        slot, col = pair * 2 + SLOT[m], COL[m]
        if at is not None:
            slot, col = at, 0
        i = m % 2
        if r == 0:
            near = [pltpu.make_async_copy(w.at[:, cols], wst.at[slot, rows(c, H), pl.ds(col + to.start, to.size)], ld.at[slot, i, j])
                    for j, (w, cols, to) in enumerate(mine(m, c))]
            return near + [pltpu.make_async_copy(bufs[m].at[partner], wst.at[slot, rows(oc, H), pl.ds(col, WID[m])], ld.at[slot, i, 2])]
        o = origin(r)
        return [pltpu.make_async_copy(bufs[m].at[2 * o + j], wst.at[slot, pl.ds(j * H, H), pl.ds(col, WID[m])], ld.at[slot, i, j]) for j in TWO]

    def load(m, r, pair):
        for cp in loads(m, r, pair):
            cp.start()

    def part(r):
        return lanes(z if r == 0 else origin(r), T)

    def multiply(m, r, pair):
        depth = part(r)

        @pl.loop(0, WID[m] // 256)
        def _(i):
            cols, to = lanes(i + COL[m] // 256, 256), lanes(i + ACC[m] // 256, 256)
            w = wst[pair * 2 + SLOT[m], :, cols]
            for j in TWO:
                at = pl.ds(j * H, H)
                got = _dot(xa[at, depth], w)
                if r == 0:
                    acc[at, to] = got
                else:
                    acc[at, to] += got

    def use(m, r, pair):
        for cp in loads(m, r, pair):
            cp.wait()
        multiply(m, r, pair)

    def project(ms, r):
        each(load, ms, r, r % 2)
        each(use, ms, r, r % 2)

    def a3_out():
        return remote(xa.at[rows(c, H)], a3.at[rows(c, H)], hs3.at[0], hr3.at[0], dp, sp - 2)

    def a3_send():
        a3_out().start()

    def a3_over(core):
        part = a3.at[rows(core, H)]
        return remote(part, part, hs3.at[1], hr3.at[1], dp, partner)

    def a3_pass():
        part = a3.at[rows(c, H)]
        remote(part, part, hs3.at[0], hr3.at[0], dp, sp).wait_recv()
        a3_over(c).start()
        a3_over(oc).wait_recv()

    def extra(r):
        pair, other = r % 2 * 2, 2 - r % 2 * 2
        copies = loads(1, r, 0, other + 1) + [pltpu.make_async_copy(a3.at[:, part(r)], wst.at[other], xl.at[9])]
        for cp in copies:
            cp.start()
        for cp in copies:
            cp.wait()
        for slot, col, to, n in ((other + 1, 0, 0, 256), (pair + 1, 512, 256, 512)):
            for j in TWO:
                at = pl.ds(j * H, H)
                got = _dot(wst[other, at, :], wst[slot, :, col : col + n])
                if r == 0:
                    eacc[at, to : to + n] = got
                else:
                    eacc[at, to : to + n] += got

    def make_extra():
        tables(3)
        ks[3, 3] = turned(eacc[:, :HEAD])
        vs[3, 3] = eacc[:, HEAD : 2 * HEAD].T.astype(BF)
        for n in FOUR:
            q_s[4, pl.ds(n * T, T), :] = turned(eacc[:, (2 + n) * HEAD : (3 + n) * HEAD])

    def finish_extra():
        for n in FOUR:
            at = pl.ds(n * T, T)
            q_s[4, at, :] = mixed(4, at)
        pl.semaphore_wait(rdy3, 1)
        for n in FOUR:
            seen3(n).start()

    def seen3(n):
        return remote(q_s.at[4, pl.ds(n * T, T)], xa.at[:, lanes(c * 16 + 12 + n, HEAD)], es.at[n], er.at[n], dp, sp + 2)

    def seen3_wait():
        for n in FOUR:
            part = xa.at[:, lanes(c * 16 + 12 + n, HEAD)]
            remote(part, part, es.at[n], er.at[n], dp, sp).wait_recv()
        seen_copy(3).start()

    def turned(t):
        t = t.astype(BF).astype(F32)
        return (t * cos_ref[...] + pltpu.roll(t, HALF, 1) * sin_ref[...]).astype(BF)

    def kv_out(d, heads):
        part = (z - d, pl.ds(0, heads))
        return [remote(b.at[part], b.at[part], cs.at[d, i], cr.at[d, i], dp, sp + 2) for i, b in enumerate((ks, vs))]

    def kv_wait(d, heads):
        part = (z - d, pl.ds(0, heads))
        for i, b in enumerate((ks, vs)):
            remote(b.at[part], b.at[part], cs.at[d - 1, i], cr.at[d - 1, i], dp, sp).wait_recv()

    def kv_start(d, heads):
        for cp in kv_out(d, heads):
            cp.start()

    def kv_send(d):
        if d < 2:
            run(z < 2, (kv_start, d, 4))
        run(is2, (kv_start, d, 3))

    def kv_pass(d):
        kv_wait(d, 4)
        kv_send(d)

    e = HEAD**-0.5 * LOG2E
    heads = 4 - half * (1 - inner)

    def block(o, head, g, keys, strips, fresh):
        k = ks[o, head, keys, :]
        scores = [_dot(k, q_s[g, pl.ds(at, STRIP), :], 1) for at, _ in strips]
        values = jnp.concatenate([vs[o, head, :, keys], jnp.ones((8, KB), BF)], axis=0)
        weights, keeps = [], []
        for (at, gap), s in zip(strips, scores):
            if gap is not None:
                ok = lax.broadcasted_iota(jnp.int32, (KB, STRIP), 1) + gap >= lax.broadcasted_iota(jnp.int32, (KB, STRIP), 0)
                s = jnp.where(ok, s, HIDDEN)
            top = s.max(axis=0, keepdims=True)
            if not fresh:
                old = top_s[g, :, pl.ds(at, STRIP)]
                top = jnp.maximum(old, top)
                keeps.append(jnp.exp2((old - top) * e))
            top_s[g, :, pl.ds(at, STRIP)] = top
            weights.append(jnp.exp2((s - top) * e).astype(BF))
        for i, ((at, _), p) in enumerate(zip(strips, weights)):
            got = _dot(values, p)
            if fresh:
                mix_s[g, :, pl.ds(at, STRIP)] = got
            else:
                mix_s[g, :, pl.ds(at, STRIP)] = mix_s[g, :, pl.ds(at, STRIP)] * keeps[i] + got

    def attend_own():
        @pl.loop(0, heads + half * inner)
        def _(g):
            o, head = z + g // 4, g - g // 4
            block(o, head, g, pl.ds(0, KB), [(at, 0 if at % T == 0 else None) for at in range(0, QS, STRIP)], True)
            block(o, head, g, pl.ds(KB, KB), [(at, 0) for at in range(STRIP, QS, T)], False)

    def mixed(g, at):
        return (mix_s[g, :HEAD, at] * (1 / mix_s[g, HEAD : HEAD + 1, at])).T.astype(BF)

    def seen_copy(g):
        cols = lanes(c * 4 + g, 512)
        return remote(xa.at[:, cols], xa.at[:, cols], hs.at[g], hr.at[g], dp, partner)

    def seen_in(g):
        cols = lanes((oc) * 4 + g, 512)
        return remote(xa.at[:, cols], xa.at[:, cols], hs.at[g], hr.at[g], dp, partner)

    barrier = pltpu.get_barrier_semaphore()
    greeted = [(dp, partner), (xd, sp), (yd, sp)]
    for d, s in greeted:
        pl.semaphore_signal(barrier, device_id={"dp": d, "sp": s}, device_id_type=MESH)
    for near, step in ((z >= 0, inward), (mid, -inward)):
        @pl.when(near)
        def _():
            for cc in TWO:
                pl.semaphore_signal(barrier, device_id={"dp": dp, "sp": (z + step) * 2 + cc}, device_id_type=MESH)
    pl.semaphore_wait(barrier, len(greeted) + 2 + 2 * inner)

    own_sends(KV, 0)
    run(mid, (own_sends, KV, 1))
    run(end, (own_sends, Q, 0))
    x_near.start()
    x_far.start()
    each(share, KV + Q)
    x_near.wait()
    x_far.wait_recv()

    def norm():
        @pl.loop(0, T // 32)
        def _(i):
            at = rows(i, 32)
            wide = xa[at, :].astype(F32)
            scale = lax.rsqrt(jnp.mean(wide * wide, -1, keepdims=True) + 1e-6)
            xa[at, :] = (wide * scale * gain_ref[...].astype(F32)[None]).astype(BF)

    norm()
    run(last, (a3_send,))
    first(KV, 1)
    run(mid, (own_sends, Q, 0), (first, KV, 2))
    each(shared_wait, KV)
    project(KV, 0)

    def tables(plane):
        @pl.loop(0, 8)
        def _(i):
            at = rows(i, 128)
            place = plane * T + i * 128 + lax.broadcasted_iota(jnp.int32, (128, HEAD), 0)
            angle = place.astype(F32) * freq_ref[...][None]
            cos_ref[at, :] = jnp.cos(angle)
            sin_ref[at, :] = jnp.sin(angle) * jnp.where(lax.broadcasted_iota(jnp.int32, (128, HEAD), 1) < HALF, -1.0, 1.0)

    tables(z)
    run(end, (first, KV, 2))
    second(KV, 1)
    first(KV, 3)
    run(mid, (own_sends, Q, 1), (relay, Q, 1))
    second(KV, 2)
    run(mid, (relay, QA, 2))
    second(KV, 3)
    run(mid, (xyforward, Q, 1), (relay, QB, 2))
    third(KV, 1)
    project(KV, 1)
    third(KV, 2)
    project(KV, 2)
    run(end, (take, QA, 1))
    third(KV, 3)
    project(KV, 3)

    def make_kv():
        def one(g, k, v):
            ks[z, g] = turned(acc[:, k : k + HEAD])
            vs[z, g] = acc[:, v : v + HEAD].T.astype(BF)

        for g in range(3):
            one(g, g * HEAD, 384 + g * HEAD)
        run(low, (one, 3, 768, 896))

    make_kv()
    run(mid, (relay, Q, 3))
    kv_send(0)
    own_sends(O, 0)
    run(mid, (own_sends, O, 1))
    run(end, (take, QB, 1))
    x_rest.start()
    for m in O:
        share(m)
    each(shared_wait, Q)
    project(Q, 0)
    run(end, (take, Q, 2))
    run(mid, (xyforward, Q, 2))
    second(Q, 1)
    run(end, (take, Q, 3))
    run(mid, (xyforward, Q, 3))
    third(Q, 1)
    project(Q, 1)
    second(Q, 2)
    run(mid, (kv_pass, 1))
    run(is2, (a3_pass,), (extra, 0), (extra, 1))
    second(Q, 3)
    third(Q, 2)
    project(Q, 2)
    run(is2, (extra, 2))
    first(O, 1)
    run(low, (first, O, 2))
    third(Q, 3)
    project(Q, 3)
    run(is2, (extra, 3))

    def ready(s, sem):
        pl.semaphore_signal(sem, device_id={"dp": dp, "sp": s}, device_id_type=MESH)

    run(last, (lambda: a3_out().wait_send(),), (ready, sp - 2, rdy3))
    ready(partner, rdy)

    def make_q():
        @pl.loop(0, heads)
        def _(g):
            for n in FOUR:
                q_s[g, pl.ds(n * T, T), :] = turned(acc[:, lanes(g * 4 + n, HEAD)])

    make_q()
    run(is2, (make_extra,), (kv_pass, 2))
    attend_own()
    second(O, 1)
    run(z < 2, (first, O, 3))
    pl.semaphore_wait(rdy, 1)

    def finish(g):
        for n in FOUR:
            at = pl.ds(n * T, T)
            xa[:, lanes(c * 16 + g * 4 + n, HEAD)] = mixed(g, at)
        seen_copy(g).start()

    def attend():
        size = 2 * heads

        @pl.loop(6 - 6 * half * inner, 6 + z * size)
        def _(i):
            other = 1 - (i + 58) // 64
            k = i - 6 + size
            d, at = k // size, k % size
            head = other * 3 + (1 - other) * (at // 2)

            @pl.when(last & (at == 0))
            def _():
                run(d == 3, (take, O, 2), (second, O, 2))
                kv_wait(d, 3)

            block(other * (2 - i // 2) + (1 - other) * (z - d), head, head + other, lanes(i % 2, KB), [(to, None) for to in range(0, QS, STRIP)], False)
            run(is2 & (i == 5), (finish_extra,), (first, O, 3))
            run((d == z) & (at % 2 == 1), (finish, at // 2))

    attend()

    def finish_all():
        pl.loop(0, 4)(finish)

    run(z == 0, (finish_all,))
    run(low, (second, O, 2))
    run(last, (seen3_wait,))
    for m in O:
        shared_wait(m)
        load(m, 0, 0)
    third(O, 1)
    for m in O:
        load(m, 1, 1)

    def seen_wait():
        for g in FOUR:
            seen_in(g).wait_recv()

    seen_wait()

    def times(r):
        for m in O:
            use(m, r, r % 2)

    times(0)
    run(last, (take, OA, 3))
    run(low, (second, OA, 3))
    third(O, 2)
    for m in O:
        load(m, 2, 0)
    times(1)
    x_rest.wait_recv()
    rest_x = [cp for h in TWO for cp in (
        pltpu.make_async_copy(x_ref.at[:, lanes(c * 2 + h, W)], wst.at[2 + h, rows(c, H)], xl.at[1 + h]),
        pltpu.make_async_copy(xp_ref.at[:, pl.ds(h * W, W)], wst.at[2 + h, rows(oc, H)], xl.at[3 + h]))]
    for cp in rest_x:
        cp.start()
    run(last, (take, OB, 3), (second, OA, 3))
    second(OB, 3)
    times(2)
    for cp in rest_x:
        cp.wait()

    def results(i):
        cols, to = pl.ds(i % 2 * 512, 512), lanes(c * 4 + i, 512)
        return (pltpu.make_async_copy(wst.at[2 + i // 2, rows(c, H), cols], y_ref.at[:, to], xl.at[5 + i]),
                remote(wst.at[2 + i // 2, rows(oc, H), cols], y_ref.at[:, to], ys.at[i], yr.at[i], dp, partner))

    def result_in(i):
        to = lanes((oc) * 4 + i, 512)
        return remote(y_ref.at[:, to], y_ref.at[:, to], ys.at[i], yr.at[i], dp, partner)

    def final(h):
        depth, m = part(3), O[h]
        third((m,), 3)
        copies = loads(m, 3, 0)
        for cp in copies:
            cp.start()
        for cp in copies:
            cp.wait()
        for i in TWO:
            for n in TWO:
                cols = slice(i * 512 + n * 256, i * 512 + n * 256 + 256)
                for j in TWO:
                    at = pl.ds(j * H, H)
                    got = acc[at, h * W + cols.start : h * W + cols.stop] + _dot(xa[at, depth], wst[h, :, cols])
                    wst[2 + h, at, cols] = (wst[2 + h, at, cols].astype(F32) + got).astype(BF)
            for cp in results(2 * h + i):
                cp.start()

    final(0)
    final(1)

    for i in FOUR:
        near, far = results(i)
        near.wait()
        far.wait_send()
        result_in(i).wait_recv()
        seen_copy(i).wait_send()
    x_far.wait_send()
    x_rest.wait_send()
    def drain(m):
        here = bufs[m].at[sp]
        remote(here, here, ps.at[2 + m], pr.at[2 + m], dp, partner).wait_send()
        for r in ROUNDS:
            for k in FOUR:
                plane(m, r, k).wait_send()

    def sent(m, k):
        quarter = bufs[m].at[sp, rows(dp, QR)]
        for cc in TWO:
            remote(quarter, quarter, so.at[m, k, cc], zr.at[m, z, c], dp, (z + (inward, -inward)[k]) * 2 + cc).wait_send()

    def forwarded(m, r):
        for cc in TWO:
            zfwd(m, r, cc).wait_send()

    each(drain, KV + Q + O)
    for m in KV + Q + O:
        sent(m, 0)
        run(mid, (forwarded, m, 1))
        run(is1 if m in SHIP else mid, (sent, m, 1), (forwarded, m, 2), (forwarded, m, 3))

    def kv_sent(d, n):
        for cp in kv_out(d, n):
            cp.wait_send()

    run(z < 2, (kv_sent, 0, 4))
    run(z == 1, (kv_sent, 1, 4))

    def plane_two():
        for d in (0, 1, 2):
            kv_sent(d, 3)
        a3_over(c).wait_send()
        for n in FOUR:
            seen3(n).wait_send()

    run(is2, (plane_two,))


def solution(mesh):
    def step(x, gain, wq, wk, wv, wo):
        freq = THETA ** (-(jnp.arange(HEAD) % (HALF)).astype(F32) / (HALF))
        far, near = pl.BlockSpec(memory_space=pl.ANY), pl.BlockSpec(memory_space=pltpu.VMEM)
        sems = pltpu.SemaphoreType.DMA
        y, *_ = pl.pallas_call(
            _layer,
            out_shape=[
                jax.ShapeDtypeStruct((H, D), BF),
                jax.ShapeDtypeStruct((H, C), BF),
                jax.ShapeDtypeStruct((T, D), BF),
                *(jax.ShapeDtypeStruct((8, H, n), BF) for n in WID),
            ],
            in_specs=[far, near, far, far, far, far, near],
            out_specs=[far] * 10,
            scratch_shapes=[
                pltpu.VMEM((T, D), BF),
                pltpu.VMEM((4, T, W), BF),
                pltpu.VMEM((T, C), F32),
                pltpu.VMEM((T, 768), F32),
                pltpu.VMEM((5, QS, HEAD), BF),
                pltpu.VMEM((4, 4, T, HEAD), BF),
                pltpu.VMEM((4, 4, HEAD, T), BF),
                pltpu.VMEM((5, HEAD + 8, QS), F32),
                pltpu.VMEM((5, 1, QS), F32),
                pltpu.VMEM((T, HEAD), F32),
                pltpu.VMEM((T, HEAD), F32),
                sems((7, 2, 2)),
                sems((7, 3, 2)),
                sems((7, 4, 2)),
                sems((7, 3, 4)),
                sems((7, 3, 4)),
                sems((3, 2)),
                sems((3, 2)),
                sems((9,)),
                sems((9,)),
                sems((4,)),
                sems((4,)),
                sems((4,)),
                sems((4,)),
                sems((4, 2, 3)),
                sems((10,)),
                sems((2,)),
                sems((2,)),
                sems((4,)),
                sems((4,)),
                pltpu.SemaphoreType.REGULAR,
                pltpu.SemaphoreType.REGULAR,
            ],
            compiler_params=pltpu.CompilerParams(collective_id=0, has_side_effects=True, vmem_limit_bytes=63 * 2**20),
        )(x, gain, wq, wk, wv, wo, freq)
        return y

    tokens, whole = P(("dp", "sp"), None), P("sp", None)
    return jax.shard_map(
        step,
        mesh=mesh,
        in_specs=(tokens, P(None), whole, whole, whole, whole),
        out_specs=tokens,
        check_vma=False,
    )
```

```python
import functools

import jax
import jax.numpy as jnp
from jax import lax
from jax.experimental import pallas as pl
from jax.experimental.pallas import tpu as pltpu
from jax.sharding import PartitionSpec as P

HEAD = 128
THETA = 10000
NEG = -1e30
HIDDEN = 2 * NEG
LOG2E = 1.4426950408889634
MESH = pl.DeviceIdType.MESH
TWO, ROUNDS, FOUR = (0, 1), (1, 2, 3), range(4)
BF = jnp.bfloat16
F32 = jnp.float32

T = 1024
D = 4096
H = 512
QR = 128
W = 1024
KV, Q, O = (0, 1), (2, 3, 4), (5, 6)
OA, OB, QA, QB = O[:1], O[1:], Q[:1], Q[1:]
WID = (768, 256, 1024, 512, 512, 1024, 1024)
SHIP = (1, 4)
ACC = (0, 768, 0, 1024, 1536, 0, 1024)
SLOT = (0, 0, 0, 1, 1, 0, 1)
COL = (0, 768, 0, 0, 512, 0, 0)
KB = 512
STRIP = 512
QS = 4 * T
HALF = HEAD // 2
C = 2048
N = 256


def _dot(a, b, cb=0):
    return lax.dot_general(a, b, (((1,), (cb,)), ((), ())), preferred_element_type=F32)


def _layer(x_ref, gain_ref, wq_ref, wk_ref, wv_ref, wo_ref, freq_ref, y_ref, xp_ref, a3, b0, b1, b2, b3, b4, b5, b6, xa, wst, acc, eacc, q_s, ks, vs, mix_s,
           top_s, cos_ref, sin_ref, so, sf, zr, fs, fr, cs, cr, ps, pr, hs, hr, ys, yr, ld, xl, hs3, hr3, es, er, rdy, rdy3):
    dp, sp = lax.axis_index("dp"), lax.axis_index("sp")
    z, c = sp // 2, sp % 2
    jx, jy = dp // 2, dp % 2
    xd, yd, diag = (1 - jx) * 2 + jy, jx * 2 + 1 - jy, 3 - dp
    half = z // 2
    inner = z + half * (3 - 2 * z)
    mid = inner == 1
    partner = z * 2 + 1 - c
    bufs = (b0, b1, b2, b3, b4, b5, b6)
    end, last, low, is1, is2 = inner == 0, z == 3, z < 3, z == 1, z == 2
    oc = 1 - c

    def run(when, *steps):
        @pl.when(when)
        def _():
            for f, *args in steps:
                f(*args)

    def each(f, ms, *args):
        for m in ms:
            if m in SHIP:
                run(low, (f, m, *args))
            else:
                f(m, *args)

    def upward(f, m, *args):
        if m in SHIP:
            run(z != 2, (f, m, *args))
        else:
            f(m, *args)

    def remote(src, dst, send, recv, d, s):
        return pltpu.make_async_remote_copy(src_ref=src, dst_ref=dst, send_sem=send, recv_sem=recv, device_id={"dp": d, "sp": s}, device_id_type=MESH)

    def lanes(i, n):
        return pl.ds(pl.multiple_of(i * n, n), n)

    def rows(i, n):
        return pl.ds(pl.multiple_of(i * n, n), n)

    def origin(r):
        base = (1 - inner, 2, 3)[r - 1]
        return base + half * (3 - 2 * base)

    def mine(m, cc):
        if m in KV:
            n, at = (384, 128)[m], cc * 512 + (0, 384)[m]
            cols = pl.ds(pl.multiple_of(at, 128), n)
            return [(wk_ref, cols, pl.ds(0, n)), (wv_ref, cols, pl.ds(n, n))]
        cols = pl.ds(pl.multiple_of(cc * C + ACC[m], H), WID[m])
        return [(wq_ref if m in Q else wo_ref, cols, pl.ds(0, WID[m]))]

    inward = 1 - 2 * half

    def own_copies(m, k, cc):
        step = (inward, -inward)[k]
        return [remote(w.at[rows(dp, QR), cols], bufs[m].at[sp, rows(dp, QR), at], so.at[m, k, cc], zr.at[m, z, c], dp, (z + step) * 2 + cc)
                for w, cols, at in mine(m, cc)]

    def own_send(m, k):
        for cc in TWO:
            for cp in own_copies(m, k, cc):
                cp.start()

    def own_sends(ms, k):
        for m in ms:
            if k:
                upward(own_send, m, k)
            else:
                own_send(m, k)

    def zfwd(m, r, cc):
        o = origin(r)
        step = (1 if r == 1 else -1) * inward
        part = bufs[m].at[2 * o + cc, rows(dp, QR)]
        return remote(part, part, sf.at[m, r - 1, cc], zr.at[m, o, cc], dp, (z + step) * 2 + c)

    def zwait(m, r):
        for cc in TWO:
            zfwd(m, r, cc).wait_recv()

    def zforward_now(m, r):
        for cc in TWO:
            zfwd(m, r, cc).start()

    def zforward(m, r):
        if r == 1:
            zforward_now(m, r)
        else:
            upward(zforward_now, m, r)

    def plane(m, r, k):
        o, b = origin(r), bufs[m]
        part = (b.at[pl.ds(2 * o, 2), rows(dp, QR)], b.at[pl.ds(2 * o, 2), rows(dp, QR)], b.at[2 * o, rows(xd, QR)], b.at[2 * o + 1, rows(yd, QR)])[k]
        return remote(part, part, fs.at[m, r - 1, k], fr.at[m, r - 1, k], (xd, yd, yd, xd)[k], sp)

    def plane_in(m, r, k):
        o, b = origin(r), bufs[m]
        part = (b.at[pl.ds(2 * o, 2), rows(xd, QR)], b.at[pl.ds(2 * o, 2), rows(yd, QR)], b.at[2 * o, rows(diag, QR)], b.at[2 * o + 1, rows(diag, QR)])[k]
        return remote(part, part, fs.at[m, r - 1, k], fr.at[m, r - 1, k], (xd, yd, yd, xd)[k], sp)

    def spread(m, r):
        plane(m, r, 0).start()
        plane(m, r, 1).start()

    def xyforward(ms, r):
        each(spread, ms, r)

    def second_one(m, r):
        plane_in(m, r, 0).wait_recv()
        plane_in(m, r, 1).wait_recv()
        plane(m, r, 2).start()
        plane(m, r, 3).start()

    def second(ms, r):
        each(second_one, ms, r)

    def third_one(m, r):
        plane_in(m, r, 2).wait_recv()
        plane_in(m, r, 3).wait_recv()

    def third(ms, r):
        each(third_one, ms, r)

    def relay(ms, r):
        for m in ms:
            zwait(m, r)
            zforward(m, r)

    def take(ms, r):
        def one(m):
            zwait(m, r)
            spread(m, r)

        each(one, ms)

    def first(ms, r):
        def one(m):
            zwait(m, r)
            run(mid, (zforward, m, r))
            spread(m, r)

        each(one, ms)

    def shared(m):
        return [remote(w.at[:, cols], bufs[m].at[sp, :, at], ps.at[2 + m], pr.at[2 + m], dp, partner) for w, cols, at in mine(m, oc)]

    def share(m):
        for cp in shared(m):
            cp.start()

    def shared_wait(m):
        part = bufs[m].at[partner]
        remote(part, part, ps.at[2 + m], pr.at[2 + m], dp, partner).wait_recv()

    x_near = pltpu.make_async_copy(x_ref, xa.at[rows(c, H)], xl.at[0])
    x_far = remote(x_ref, xa.at[rows(c, H)], ps.at[0], pr.at[0], dp, partner)
    x_rest = remote(x_ref.at[:, lanes(oc, C)], xp_ref, ps.at[1], pr.at[1], dp, partner)

    def loads(m, r, pair, at=None):
        slot, col = pair * 2 + SLOT[m], COL[m]
        if at is not None:
            slot, col = at, 0
        i = m % 2
        if r == 0:
            near = [pltpu.make_async_copy(w.at[:, cols], wst.at[slot, rows(c, H), pl.ds(col + to.start, to.size)], ld.at[slot, i, j])
                    for j, (w, cols, to) in enumerate(mine(m, c))]
            return near + [pltpu.make_async_copy(bufs[m].at[partner], wst.at[slot, rows(oc, H), pl.ds(col, WID[m])], ld.at[slot, i, 2])]
        o = origin(r)
        return [pltpu.make_async_copy(bufs[m].at[2 * o + j], wst.at[slot, pl.ds(j * H, H), pl.ds(col, WID[m])], ld.at[slot, i, j]) for j in TWO]

    def own_output(m):
        (w, cols, _), = mine(m, c)
        return pltpu.make_async_copy(w.at[:, cols], bufs[m].at[sp], xl.at[5 + m])

    def load(m, r, pair):
        for cp in loads(m, r, pair):
            cp.start()

    def part(r):
        return lanes(z if r == 0 else origin(r), T)

    def multiply(m, r, pair, depth=None):
        depth = part(r) if depth is None else depth

        @pl.loop(0, WID[m] // N)
        def _(i):
            cols, to = lanes(i + COL[m] // N, N), lanes(i + ACC[m] // N, N)
            w = wst[pair * 2 + SLOT[m], :, cols]
            for j in TWO:
                at = pl.ds(j * H, H)
                got = _dot(xa[at, depth], w)
                if r == 0:
                    acc[at, to] = got
                else:
                    acc[at, to] += got

    def use(m, r, pair):
        for cp in loads(m, r, pair):
            cp.wait()
        multiply(m, r, pair)

    def project(ms, r):
        each(load, ms, r, r % 2)
        each(use, ms, r, r % 2)

    def a3_out():
        return remote(xa.at[rows(c, H)], a3.at[rows(c, H)], hs3.at[0], hr3.at[0], dp, sp - 2)

    def a3_send():
        a3_out().start()

    def a3_over(core):
        part = a3.at[rows(core, H)]
        return remote(part, part, hs3.at[1], hr3.at[1], dp, partner)

    def a3_pass():
        part = a3.at[rows(c, H)]
        remote(part, part, hs3.at[0], hr3.at[0], dp, sp).wait_recv()
        a3_over(c).start()
        a3_over(oc).wait_recv()

    def extra(r):
        pair, other = r % 2 * 2, 2 - r % 2 * 2
        copies = loads(1, r, 0, other + 1) + [pltpu.make_async_copy(a3.at[:, part(r)], wst.at[other], xl.at[9])]
        for cp in copies:
            cp.start()
        for cp in copies:
            cp.wait()
        for slot, col, to, n in ((other + 1, 0, 0, N), (pair + 1, 512, 256, H)):
            for j in TWO:
                at = pl.ds(j * H, H)
                got = _dot(wst[other, at, :], wst[slot, :, col : col + n])
                if r == 0:
                    eacc[at, to : to + n] = got
                else:
                    eacc[at, to : to + n] += got

    def make_extra():
        tables(3)
        ks[3, 3] = turned(eacc[:, :HEAD])
        vs[3, 3] = eacc[:, HEAD : 2 * HEAD].T.astype(BF)
        for n in FOUR:
            q_s[4, pl.ds(n * T, T), :] = turned(eacc[:, (2 + n) * HEAD : (3 + n) * HEAD])

    def finish_extra():
        for n in FOUR:
            at = pl.ds(n * T, T)
            q_s[4, at, :] = mixed(4, at)
        pl.semaphore_wait(rdy3, 1)
        for n in FOUR:
            seen3(n).start()

    def seen3(n):
        return remote(q_s.at[4, pl.ds(n * T, T)], xa.at[:, lanes(c * 16 + 12 + n, HEAD)], es.at[n], er.at[n], dp, sp + 2)

    def seen3_wait():
        for n in FOUR:
            part = xa.at[:, lanes(c * 16 + 12 + n, HEAD)]
            remote(part, part, es.at[n], er.at[n], dp, sp).wait_recv()
        seen_copy(3).start()

    def turned(t):
        t = t.astype(BF).astype(F32)
        return (t * cos_ref[...] + pltpu.roll(t, HALF, 1) * sin_ref[...]).astype(BF)

    def kv_out(d, heads):
        part = (z - d, pl.ds(0, heads))
        return [remote(b.at[part], b.at[part], cs.at[d, i], cr.at[d, i], dp, sp + 2) for i, b in enumerate((ks, vs))]

    def kv_wait(d, heads):
        part = (z - d, pl.ds(0, heads))
        for i, b in enumerate((ks, vs)):
            remote(b.at[part], b.at[part], cs.at[d - 1, i], cr.at[d - 1, i], dp, sp).wait_recv()

    def kv_start(d, heads):
        for cp in kv_out(d, heads):
            cp.start()

    def kv_send(d):
        if d < 2:
            run(z < 2, (kv_start, d, 4))
        run(is2, (kv_start, d, 3))

    def kv_pass(d):
        kv_wait(d, 4)
        kv_send(d)

    e = HEAD**-0.5 * LOG2E
    heads = 4 - half * (1 - inner)

    def block(o, head, g, keys, strips, fresh):
        k = ks[o, head, keys, :]
        scores = [_dot(k, q_s[g, pl.ds(at, STRIP), :], 1) for at, _ in strips]
        values = jnp.concatenate([vs[o, head, :, keys], jnp.ones((8, KB), BF)], axis=0)
        weights, keeps = [], []
        for (at, gap), s in zip(strips, scores):
            if gap is not None:
                ok = lax.broadcasted_iota(jnp.int32, (KB, STRIP), 1) + gap >= lax.broadcasted_iota(jnp.int32, (KB, STRIP), 0)
                s = jnp.where(ok, s, HIDDEN)
            top = s.max(axis=0, keepdims=True)
            if not fresh:
                old = top_s[g, :, pl.ds(at, STRIP)]
                top = jnp.maximum(old, top)
                keeps.append(jnp.exp2((old - top) * e))
            top_s[g, :, pl.ds(at, STRIP)] = top
            weights.append(jnp.exp2((s - top) * e).astype(BF))
        for i, ((at, _), p) in enumerate(zip(strips, weights)):
            got = _dot(values, p)
            if fresh:
                mix_s[g, :, pl.ds(at, STRIP)] = got
            else:
                mix_s[g, :, pl.ds(at, STRIP)] = mix_s[g, :, pl.ds(at, STRIP)] * keeps[i] + got

    def attend_own():
        @pl.loop(0, heads + half * inner)
        def _(g):
            o, head = z + g // 4, g - g // 4
            block(o, head, g, pl.ds(0, KB), [(at, 0 if at % T == 0 else None) for at in range(0, QS, STRIP)], True)
            block(o, head, g, pl.ds(KB, KB), [(at, 0) for at in range(STRIP, QS, T)], False)

    def mixed(g, at):
        return (mix_s[g, :HEAD, at] * (1 / mix_s[g, HEAD : HEAD + 1, at])).T.astype(BF)

    def seen_copy(g):
        cols = lanes(c * 4 + g, H)
        return remote(xa.at[:, cols], xa.at[:, cols], hs.at[g], hr.at[g], dp, partner)

    def seen_in(g):
        cols = lanes((oc) * 4 + g, H)
        return remote(xa.at[:, cols], xa.at[:, cols], hs.at[g], hr.at[g], dp, partner)

    barrier = pltpu.get_barrier_semaphore()
    greeted = [(dp, partner), (xd, sp), (yd, sp)]
    for d, s in greeted:
        pl.semaphore_signal(barrier, device_id={"dp": d, "sp": s}, device_id_type=MESH)
    for near, step in ((z >= 0, inward), (mid, -inward)):
        @pl.when(near)
        def _():
            for cc in TWO:
                pl.semaphore_signal(barrier, device_id={"dp": dp, "sp": (z + step) * 2 + cc}, device_id_type=MESH)
    pl.semaphore_wait(barrier, len(greeted) + 2 + 2 * inner)

    own_sends(KV, 0)
    run(mid, (own_sends, KV, 1))
    run(is2, (own_sends, Q, 1))
    run(end, (own_sends, Q, 0))
    x_near.start()
    x_far.start()
    each(share, KV + Q)
    x_near.wait()
    x_far.wait_recv()

    def norm():
        @pl.loop(0, T // 32)
        def _(i):
            at = rows(i, 32)
            wide = xa[at, :].astype(F32)
            scale = lax.rsqrt(jnp.mean(wide * wide, -1, keepdims=True) + 1e-6)
            xa[at, :] = (wide * scale * gain_ref[...].astype(F32)[None]).astype(BF)

    norm()
    run(last, (a3_send,))
    first(KV, 1)
    run(mid, (own_sends, Q, 0), (first, KV, 2))
    each(shared_wait, KV)
    project(KV, 0)

    def tables(plane):
        @pl.loop(0, 8)
        def _(i):
            at = rows(i, 128)
            place = plane * T + i * 128 + lax.broadcasted_iota(jnp.int32, (128, HEAD), 0)
            angle = place.astype(F32) * freq_ref[...][None]
            cos_ref[at, :] = jnp.cos(angle)
            sin_ref[at, :] = jnp.sin(angle) * jnp.where(lax.broadcasted_iota(jnp.int32, (128, HEAD), 1) < HALF, -1.0, 1.0)

    tables(z)
    run(end, (first, KV, 2))
    second(KV, 1)
    first(KV, 3)
    run(z == 1, (own_sends, Q, 1))
    run(mid, (relay, Q, 1))
    second(KV, 2)
    run(mid, (relay, QA, 2))
    second(KV, 3)
    run(mid, (xyforward, Q, 1), (relay, QB, 2))
    run(is2, (own_sends, OA, 1))
    third(KV, 1)
    project(KV, 1)
    third(KV, 2)
    project(KV, 2)
    run(end, (take, QA, 1))
    third(KV, 3)
    project(KV, 3)

    def make_kv():
        def one(g, k, v):
            ks[z, g] = turned(acc[:, k : k + HEAD])
            vs[z, g] = acc[:, v : v + HEAD].T.astype(BF)

        for g in range(3):
            one(g, g * HEAD, 384 + g * HEAD)
        run(low, (one, 3, 768, 896))

    make_kv()
    run(mid, (relay, Q, 3))
    kv_send(0)
    own_sends(O, 0)
    run(z == 1, (own_sends, O, 1))
    run(is2, (own_sends, OB, 1))
    run(end, (take, QB, 1))
    x_rest.start()
    for m in O:
        share(m)
        own_output(m).start()
    each(shared_wait, Q)
    project(Q, 0)
    run(end, (take, Q, 2))
    run(mid, (xyforward, Q, 2))
    second(Q, 1)
    run(end, (take, Q, 3))
    run(mid, (xyforward, Q, 3))
    third(Q, 1)
    project(Q, 1)
    second(Q, 2)
    run(is2, (kv_pass, 1))
    run(is2, (a3_pass,), (extra, 0), (extra, 1))
    second(Q, 3)
    run(z == 1, (relay, O, 1), (kv_pass, 1))
    third(Q, 2)
    project(Q, 2)
    run(is2, (extra, 2))
    run(z != 1, (first, O, 1))
    run(z == 1, (xyforward, O, 1))
    run(low, (first, O, 2))
    third(Q, 3)
    project(Q, 3)
    run(is2, (extra, 3))

    def ready(s, sem):
        pl.semaphore_signal(sem, device_id={"dp": dp, "sp": s}, device_id_type=MESH)

    run(last, (lambda: a3_out().wait_send(),), (ready, sp - 2, rdy3))
    ready(partner, rdy)

    def make_q():
        @pl.loop(0, heads)
        def _(g):
            for n in FOUR:
                q_s[g, pl.ds(n * T, T), :] = turned(acc[:, lanes(g * 4 + n, HEAD)])

    make_q()
    run(is2, (make_extra,), (first, O, 3))
    attend_own()
    second(O, 1)
    run(z < 2, (first, O, 3))
    pl.semaphore_wait(rdy, 1)

    def finish(g):
        for n in FOUR:
            at = pl.ds(n * T, T)
            xa[:, lanes(c * 16 + g * 4 + n, HEAD)] = mixed(g, at)
        seen_copy(g).start()

    whole = [(at, None) for at in range(0, QS, STRIP)]

    def attend():
        size = 2 * heads

        @pl.loop(6 - 6 * half * inner, 6 + z * size)
        def _(i):
            other = 1 - (i + 58) // 64
            k = i - 6 + size
            d, at = k // size, k % size
            head = other * 3 + (1 - other) * (at // 2)

            @pl.when(last & (at == 0))
            def _():
                run(d == 3, (take, O, 2), (take, O, 3), (second, O, 2), (second, O, 3))
                kv_wait(d, 3)
            run(is2 & (i == 4), (kv_pass, 2))

            block(other * (2 - i // 2) + (1 - other) * (z - d), head, head + other, lanes(i % 2, KB), whole, False)
            run(is2 & (i == 5), (finish_extra,), (second, O, 2))
            run(is2 & (i == 13), (second, O, 3))
            run((d == z) & (at % 2 == 1), (finish, at // 2))

    attend()

    def finish_all():
        pl.loop(0, 4)(finish)

    run(z == 0, (finish_all,))
    run(z < 2, (second, O, 2))
    run(last, (third, O, 1), (third, O, 2), (third, O, 3))
    swap = z // 3
    order = [o + swap * (p - o) for o, p in zip([z] + [origin(r) for r in ROUNDS], (2, 0, 3, 1))]

    def slot(m, i):
        return i % 2 * 2 + SLOT[m]

    def output_loads(m, i):
        return [pltpu.make_async_copy(bufs[m].at[2 * order[i] + j], wst.at[slot(m, i), pl.ds(j * H, H)], ld.at[slot(m, i), 0, j]) for j in TWO]

    def output_load(i):
        for m in O:
            for cp in output_loads(m, i):
                cp.start()

    def output(i):
        for m in O:
            for cp in output_loads(m, i):
                cp.wait()
            multiply(m, i, i % 2, lanes(order[i], T))

    def seen_wait(*gs):
        for g in gs:
            seen_in(g).wait_recv()

    for m in O:
        shared_wait(m)
        own_output(m).wait()
    output_load(0)
    run(low, (third, O, 1))
    output_load(1)
    seen_wait(*TWO)
    run(z == 1, (seen_wait, 2, 3))
    output(0)
    run(z != 1, (seen_wait, 2))
    run(z % 2 == 0, (seen_wait, 3))
    run(z < 2, (second, OA, 3))
    run(low, (third, O, 2))
    output_load(2)
    output(1)
    x_rest.wait_recv()
    rest_x = [cp for h in TWO for cp in (
        pltpu.make_async_copy(x_ref.at[:, lanes(c * 2 + h, W)], wst.at[2 + h, rows(c, H)], xl.at[1 + h]),
        pltpu.make_async_copy(xp_ref.at[:, pl.ds(h * W, W)], wst.at[2 + h, rows(oc, H)], xl.at[3 + h]))]
    for cp in rest_x:
        cp.start()
    run(z < 2, (second, OB, 3))
    run(last, (seen3_wait,), (seen_wait, 3))
    output(2)
    for cp in rest_x:
        cp.wait()

    def results(i):
        cols, to = pl.ds(i % 2 * 512, H), lanes(c * 4 + i, H)
        return (pltpu.make_async_copy(wst.at[2 + i // 2, rows(c, H), cols], y_ref.at[:, to], xl.at[5 + i]),
                remote(wst.at[2 + i // 2, rows(oc, H), cols], y_ref.at[:, to], ys.at[i], yr.at[i], dp, partner))

    def result_in(i):
        to = lanes((oc) * 4 + i, H)
        return remote(y_ref.at[:, to], y_ref.at[:, to], ys.at[i], yr.at[i], dp, partner)

    def final(h):
        depth, m = lanes(order[3], T), O[h]
        run(low, (third, (m,), 3))
        copies = [pltpu.make_async_copy(bufs[m].at[2 * order[3] + j], wst.at[h, pl.ds(j * H, H)], ld.at[h, 0, j]) for j in TWO]
        for cp in copies:
            cp.start()
        for cp in copies:
            cp.wait()
        for i in TWO:
            for n in TWO:
                cols = slice(i * 512 + n * 256, i * 512 + n * 256 + 256)
                for j in TWO:
                    at = pl.ds(j * H, H)
                    got = acc[at, h * W + cols.start : h * W + cols.stop] + _dot(xa[at, depth], wst[h, :, cols])
                    wst[2 + h, at, cols] = (wst[2 + h, at, cols].astype(F32) + got).astype(BF)
            for cp in results(2 * h + i):
                cp.start()

    final(0)
    final(1)

    for i in FOUR:
        near, far = results(i)
        near.wait()
        far.wait_send()
        result_in(i).wait_recv()
        seen_copy(i).wait_send()
    x_far.wait_send()
    x_rest.wait_send()
    def drain(m):
        here = bufs[m].at[sp]
        remote(here, here, ps.at[2 + m], pr.at[2 + m], dp, partner).wait_send()
        for r in ROUNDS:
            for k in FOUR:
                plane(m, r, k).wait_send()

    def sent(m, k):
        quarter = bufs[m].at[sp, rows(dp, QR)]
        for cc in TWO:
            remote(quarter, quarter, so.at[m, k, cc], zr.at[m, z, c], dp, (z + (inward, -inward)[k]) * 2 + cc).wait_send()

    def forwarded(m, r):
        for cc in TWO:
            zfwd(m, r, cc).wait_send()

    each(drain, KV + Q + O)
    for m in KV + Q + O:
        sent(m, 0)
        run(mid, (forwarded, m, 1))
        run(is1 if m in SHIP else mid, (sent, m, 1), (forwarded, m, 2), (forwarded, m, 3))

    def kv_sent(d, n):
        for cp in kv_out(d, n):
            cp.wait_send()

    run(z < 2, (kv_sent, 0, 4))
    run(z == 1, (kv_sent, 1, 4))

    def plane_two():
        for d in range(3):
            kv_sent(d, 3)
        a3_over(c).wait_send()
        for n in FOUR:
            seen3(n).wait_send()

    run(is2, (plane_two,))


def solution(mesh):
    def step(x, gain, wq, wk, wv, wo):
        freq = THETA ** (-(jnp.arange(HEAD) % (HALF)).astype(F32) / (HALF))
        far, near = pl.BlockSpec(memory_space=pl.ANY), pl.BlockSpec(memory_space=pltpu.VMEM)
        sems = pltpu.SemaphoreType.DMA
        y, *_ = pl.pallas_call(
            _layer,
            out_shape=[
                jax.ShapeDtypeStruct((H, D), BF),
                jax.ShapeDtypeStruct((H, C), BF),
                jax.ShapeDtypeStruct((T, D), BF),
                *(jax.ShapeDtypeStruct((8, H, n), BF) for n in WID),
            ],
            in_specs=[far, near, far, far, far, far, near],
            out_specs=[far] * 10,
            scratch_shapes=[
                pltpu.VMEM((T, D), BF),
                pltpu.VMEM((4, T, W), BF),
                pltpu.VMEM((T, C), F32),
                pltpu.VMEM((T, 768), F32),
                pltpu.VMEM((5, QS, HEAD), BF),
                pltpu.VMEM((4, 4, T, HEAD), BF),
                pltpu.VMEM((4, 4, HEAD, T), BF),
                pltpu.VMEM((5, HEAD + 8, QS), F32),
                pltpu.VMEM((5, 1, QS), F32),
                pltpu.VMEM((T, HEAD), F32),
                pltpu.VMEM((T, HEAD), F32),
                sems((7, 2, 2)),
                sems((7, 3, 2)),
                sems((7, 4, 2)),
                *[sems((7, 3, 4))] * 2,
                *[sems((3, 2))] * 2,
                *[sems((9,))] * 2,
                *[sems((4,))] * 4,
                sems((4, 2, 3)),
                sems((12,)),
                *[sems((2,))] * 2,
                *[sems((4,))] * 2,
                *[pltpu.SemaphoreType.REGULAR] * 2,
            ],
            compiler_params=pltpu.CompilerParams(collective_id=0, has_side_effects=True, vmem_limit_bytes=63 * 2**20),
        )(x, gain, wq, wk, wv, wo, freq)
        return y

    tokens, whole = P(("dp", "sp")), P("sp")
    return jax.shard_map(
        step,
        mesh=mesh,
        in_specs=(tokens, P(), whole, whole, whole, whole),
        out_specs=tokens,
        check_vma=False,
    )
```

```python
import functools

import jax
import jax.numpy as jnp
from jax import lax
from jax.experimental import pallas as pl
from jax.experimental.pallas import tpu as pltpu
from jax.sharding import PartitionSpec as P

HEAD = 128
THETA = 10000
NEG = -1e30
HIDDEN = 2 * NEG
LOG2E = 1.4426950408889634
MESH = pl.DeviceIdType.MESH
TWO, ROUNDS, FOUR = (0, 1), (1, 2, 3), range(4)
BF = jnp.bfloat16
F32 = jnp.float32

T = 1024
D = 4096
H = 512
QR = 128
W = 1024
KV, Q, O = (0, 1), (2, 3, 4), (5, 6)
OA, OB, QA, QB = O[:1], O[1:], Q[:1], Q[1:]
WID = (768, 256, 1024, 512, 512, 1024, 1024)
SHIP = (1, 4)
ACC = (0, 768, 0, 1024, 1536, 0, 1024)
SLOT = (0, 0, 0, 1, 1, 0, 1)
COL = (0, 768, 0, 0, 512, 0, 0)
KB = 512
STRIP = 512
QS = 4 * T
HALF = HEAD // 2
C = 2048
N = 256


def _dot(a, b, cb=0):
    return lax.dot_general(a, b, (((1,), (cb,)), ((), ())), preferred_element_type=F32)


def _layer(x_ref, gain_ref, wq_ref, wk_ref, wv_ref, wo_ref, freq_ref, y_ref, xp_ref, a3, b0, b1, b2, b3, b4, b5, b6, xa, wst, acc, eacc, q_s, ks, vs, mix_s,
           top_s, cos_ref, sin_ref, so, sf, zr, fs, fr, cs, cr, ps, pr, hs, hr, ys, yr, ld, xl, hs3, hr3, es, er, rdy, rdy3):
    dp, sp = lax.axis_index("dp"), lax.axis_index("sp")
    z, c = sp // 2, sp % 2
    jx, jy = dp // 2, dp % 2
    xd, yd, diag = (1 - jx) * 2 + jy, jx * 2 + 1 - jy, 3 - dp
    half = z // 2
    inner = z + half * (3 - 2 * z)
    mid = inner == 1
    partner = z * 2 + 1 - c
    bufs = (b0, b1, b2, b3, b4, b5, b6)
    end, last, low, is1, is2 = inner == 0, z == 3, z < 3, z == 1, z == 2
    oc = 1 - c

    def run(when, *steps):
        @pl.when(when)
        def _():
            for f, *args in steps:
                f(*args)

    def each(f, ms, *args):
        for m in ms:
            if m in SHIP:
                run(low, (f, m, *args))
            else:
                f(m, *args)

    def upward(f, m, *args):
        if m in SHIP:
            run(z != 2, (f, m, *args))
        else:
            f(m, *args)

    def remote(src, dst, send, recv, d, s):
        return pltpu.make_async_remote_copy(src_ref=src, dst_ref=dst, send_sem=send, recv_sem=recv, device_id={"dp": d, "sp": s}, device_id_type=MESH)

    def lanes(i, n):
        return pl.ds(pl.multiple_of(i * n, n), n)

    def rows(i, n):
        return pl.ds(pl.multiple_of(i * n, n), n)

    def origin(r):
        base = (1 - inner, 2, 3)[r - 1]
        return base + half * (3 - 2 * base)

    def mine(m, cc):
        if m in KV:
            n, at = (384, 128)[m], cc * 512 + (0, 384)[m]
            cols = pl.ds(pl.multiple_of(at, 128), n)
            return [(wk_ref, cols, pl.ds(0, n)), (wv_ref, cols, pl.ds(n, n))]
        cols = pl.ds(pl.multiple_of(cc * C + ACC[m], H), WID[m])
        return [(wq_ref if m in Q else wo_ref, cols, pl.ds(0, WID[m]))]

    inward = 1 - 2 * half

    def own_copies(m, k, cc):
        step = (inward, -inward)[k]
        return [remote(w.at[rows(dp, QR), cols], bufs[m].at[sp, rows(dp, QR), at], so.at[m, k, cc], zr.at[m, z, c], dp, (z + step) * 2 + cc)
                for w, cols, at in mine(m, cc)]

    def own_send(m, k):
        for cc in TWO:
            for cp in own_copies(m, k, cc):
                cp.start()

    def own_sends(ms, k):
        for m in ms:
            if k:
                upward(own_send, m, k)
            else:
                own_send(m, k)

    def zfwd(m, r, cc):
        o = origin(r)
        step = (1 if r == 1 else -1) * inward
        part = bufs[m].at[2 * o + cc, rows(dp, QR)]
        return remote(part, part, sf.at[m, r - 1, cc], zr.at[m, o, cc], dp, (z + step) * 2 + c)

    def zwait(m, r):
        for cc in TWO:
            zfwd(m, r, cc).wait_recv()

    def zforward_now(m, r):
        for cc in TWO:
            zfwd(m, r, cc).start()

    def zforward(m, r):
        if r == 1:
            zforward_now(m, r)
        else:
            upward(zforward_now, m, r)

    def plane(m, r, k):
        o, b = origin(r), bufs[m]
        part = (b.at[pl.ds(2 * o, 2), rows(dp, QR)], b.at[pl.ds(2 * o, 2), rows(dp, QR)], b.at[2 * o, rows(xd, QR)], b.at[2 * o + 1, rows(yd, QR)])[k]
        return remote(part, part, fs.at[m, r - 1, k], fr.at[m, r - 1, k], (xd, yd, yd, xd)[k], sp)

    def plane_in(m, r, k):
        o, b = origin(r), bufs[m]
        part = (b.at[pl.ds(2 * o, 2), rows(xd, QR)], b.at[pl.ds(2 * o, 2), rows(yd, QR)], b.at[2 * o, rows(diag, QR)], b.at[2 * o + 1, rows(diag, QR)])[k]
        return remote(part, part, fs.at[m, r - 1, k], fr.at[m, r - 1, k], (xd, yd, yd, xd)[k], sp)

    def spread(m, r):
        plane(m, r, 0).start()
        plane(m, r, 1).start()

    def xyforward(ms, r):
        each(spread, ms, r)

    def second_one(m, r):
        plane_in(m, r, 0).wait_recv()
        plane_in(m, r, 1).wait_recv()
        plane(m, r, 2).start()
        plane(m, r, 3).start()

    def second(ms, r):
        each(second_one, ms, r)

    def third_one(m, r):
        plane_in(m, r, 2).wait_recv()
        plane_in(m, r, 3).wait_recv()

    def third(ms, r):
        each(third_one, ms, r)

    def relay(ms, r):
        for m in ms:
            zwait(m, r)
            zforward(m, r)

    def take(ms, r):
        def one(m):
            zwait(m, r)
            spread(m, r)

        each(one, ms)

    def first(ms, r):
        def one(m):
            zwait(m, r)
            run(mid, (zforward, m, r))
            spread(m, r)

        each(one, ms)

    def shared(m):
        return [remote(w.at[:, cols], bufs[m].at[sp, :, at], ps.at[2 + m], pr.at[2 + m], dp, partner) for w, cols, at in mine(m, oc)]

    def share(m):
        for cp in shared(m):
            cp.start()

    def shared_wait(m):
        part = bufs[m].at[partner]
        remote(part, part, ps.at[2 + m], pr.at[2 + m], dp, partner).wait_recv()

    x_near = pltpu.make_async_copy(x_ref, xa.at[rows(c, H)], xl.at[0])
    x_far = remote(x_ref, xa.at[rows(c, H)], ps.at[0], pr.at[0], dp, partner)
    x_rest = remote(x_ref.at[:, lanes(oc, C)], xp_ref, ps.at[1], pr.at[1], dp, partner)

    def loads(m, r, pair, at=None):
        slot, col = pair * 2 + SLOT[m], COL[m]
        if at is not None:
            slot, col = at, 0
        i = m % 2
        if r == 0:
            near = [pltpu.make_async_copy(w.at[:, cols], wst.at[slot, rows(c, H), pl.ds(col + to.start, to.size)], ld.at[slot, i, j])
                    for j, (w, cols, to) in enumerate(mine(m, c))]
            return near + [pltpu.make_async_copy(bufs[m].at[partner], wst.at[slot, rows(oc, H), pl.ds(col, WID[m])], ld.at[slot, i, 2])]
        o = origin(r)
        return [pltpu.make_async_copy(bufs[m].at[2 * o + j], wst.at[slot, pl.ds(j * H, H), pl.ds(col, WID[m])], ld.at[slot, i, j]) for j in TWO]

    def own_output(m):
        (w, cols, _), = mine(m, c)
        return pltpu.make_async_copy(w.at[:, cols], bufs[m].at[sp], xl.at[5 + m])

    def load(m, r, pair):
        for cp in loads(m, r, pair):
            cp.start()

    def part(r):
        return lanes(z if r == 0 else origin(r), T)

    def multiply(m, r, pair, depth=None):
        depth = part(r) if depth is None else depth

        @pl.loop(0, WID[m] // N)
        def _(i):
            cols, to = lanes(i + COL[m] // N, N), lanes(i + ACC[m] // N, N)
            w = wst[pair * 2 + SLOT[m], :, cols]
            for j in TWO:
                at = pl.ds(j * H, H)
                got = _dot(xa[at, depth], w)
                if r == 0:
                    acc[at, to] = got
                else:
                    acc[at, to] += got

    def use(m, r, pair):
        for cp in loads(m, r, pair):
            cp.wait()
        multiply(m, r, pair)

    def fetch(m, r, pair):
        if r:
            third_one(m, r)
        load(m, r, pair)

    def project(ms, r):
        each(fetch, ms, r, r % 2)
        each(use, ms, r, r % 2)

    def a3_out():
        return remote(xa.at[rows(c, H)], a3.at[rows(c, H)], hs3.at[0], hr3.at[0], dp, sp - 2)

    def a3_send():
        a3_out().start()

    def a3_over(core):
        part = a3.at[rows(core, H)]
        return remote(part, part, hs3.at[1], hr3.at[1], dp, partner)

    def a3_pass():
        part = a3.at[rows(c, H)]
        remote(part, part, hs3.at[0], hr3.at[0], dp, sp).wait_recv()
        a3_over(c).start()
        a3_over(oc).wait_recv()

    def extra(r):
        pair, other = r % 2 * 2, 2 - r % 2 * 2
        copies = loads(1, r, 0, other + 1) + [pltpu.make_async_copy(a3.at[:, part(r)], wst.at[other], xl.at[9])]
        for cp in copies:
            cp.start()
        for cp in copies:
            cp.wait()
        for slot, col, to, n in ((other + 1, 0, 0, N), (pair + 1, 512, 256, H)):
            for j in TWO:
                at = pl.ds(j * H, H)
                got = _dot(wst[other, at, :], wst[slot, :, col : col + n])
                if r == 0:
                    eacc[at, to : to + n] = got
                else:
                    eacc[at, to : to + n] += got

    def make_extra():
        ks[3, 3] = turned(eacc[:, :HEAD], 1)
        vs[3, 3] = eacc[:, HEAD : 2 * HEAD].T.astype(BF)
        for n in FOUR:
            q_s[4, pl.ds(n * T, T), :] = turned(eacc[:, lanes(2 + n, HEAD)], 1)

    def finish_extra():
        for n in FOUR:
            at = pl.ds(n * T, T)
            q_s[4, at, :] = mixed(4, at)
        pl.semaphore_wait(rdy3, 1)
        for n in FOUR:
            seen3(n).start()

    def seen3(n):
        return remote(q_s.at[4, pl.ds(n * T, T)], xa.at[:, lanes(c * 16 + 12 + n, HEAD)], es.at[n], er.at[n], dp, sp + 2)

    def seen3_wait():
        for n in FOUR:
            part = xa.at[:, lanes(c * 16 + 12 + n, HEAD)]
            remote(part, part, es.at[n], er.at[n], dp, sp).wait_recv()
        seen_copy(3).start()

    def turned(t, k=0):
        t = t.astype(BF).astype(F32)
        return (t * cos_ref[k] + pltpu.roll(t, HALF, 1) * sin_ref[k]).astype(BF)

    def kv_out(d, heads):
        return [remote(b.at[z - d, g], b.at[z - d, g], cs.at[d, g, i], cr.at[d, g, i], dp, sp + 2) for g in range(heads) for i, b in enumerate((ks, vs))]

    def kv_take(d, g):
        for i, b in enumerate((ks, vs)):
            remote(b.at[z - d, g], b.at[z - d, g], cs.at[d - 1, g, i], cr.at[d - 1, g, i], dp, sp).wait_recv()

    def kv_start(d, heads):
        for cp in kv_out(d, heads):
            cp.start()

    def kv_send(d):
        if d < 2:
            run(z < 2, (kv_start, d, 4))
        run(is2, (kv_start, d, 3))

    def kv_pass(d):
        for g in FOUR:
            kv_take(d, g)
        kv_send(d)

    e = HEAD**-0.5 * LOG2E
    heads = 4 - half * (1 - inner)

    def block(o, head, g, keys, strips, fresh):
        k = ks[o, head, keys, :]
        scores = [_dot(k, q_s[g, pl.ds(at, STRIP), :], 1) for at, _ in strips]
        values = jnp.concatenate([vs[o, head, :, keys], jnp.ones((8, KB), BF)], axis=0)
        weights, keeps = [], []
        for (at, gap), s in zip(strips, scores):
            if gap is not None:
                ok = lax.broadcasted_iota(jnp.int32, (KB, STRIP), 1) + gap >= lax.broadcasted_iota(jnp.int32, (KB, STRIP), 0)
                s = jnp.where(ok, s, HIDDEN)
            top = s.max(axis=0, keepdims=True)
            if not fresh:
                old = top_s[g, :, pl.ds(at, STRIP)]
                top = jnp.maximum(old, top)
                keeps.append(jnp.exp2((old - top) * e))
            top_s[g, :, pl.ds(at, STRIP)] = top
            weights.append(jnp.exp2((s - top) * e).astype(BF))
        for i, ((at, _), p) in enumerate(zip(strips, weights)):
            got = _dot(values, p)
            if fresh:
                mix_s[g, :, pl.ds(at, STRIP)] = got
            else:
                mix_s[g, :, pl.ds(at, STRIP)] = mix_s[g, :, pl.ds(at, STRIP)] * keeps[i] + got

    def attend_own():
        @pl.loop(0, heads + half * inner)
        def _(g):
            o, head = z + g // 4, g - g // 4
            block(o, head, g, pl.ds(0, KB), [(at, 0 if at % T == 0 else None) for at in range(0, QS, STRIP)], True)
            block(o, head, g, pl.ds(KB, KB), [(at, 0) for at in range(STRIP, QS, T)], False)

    def mixed(g, at):
        return (mix_s[g, :HEAD, at] * (1 / mix_s[g, HEAD : HEAD + 1, at])).T.astype(BF)

    def seen_copy(g):
        cols = lanes(c * 4 + g, H)
        return remote(xa.at[:, cols], xa.at[:, cols], hs.at[g], hr.at[g], dp, partner)

    def seen_in(g):
        cols = lanes((oc) * 4 + g, H)
        return remote(xa.at[:, cols], xa.at[:, cols], hs.at[g], hr.at[g], dp, partner)

    barrier = pltpu.get_barrier_semaphore()
    greeted = [(dp, partner), (xd, sp), (yd, sp)]
    for d, s in greeted:
        pl.semaphore_signal(barrier, device_id={"dp": d, "sp": s}, device_id_type=MESH)
    for near, step in ((z >= 0, inward), (mid, -inward)):
        @pl.when(near)
        def _():
            for cc in TWO:
                pl.semaphore_signal(barrier, device_id={"dp": dp, "sp": (z + step) * 2 + cc}, device_id_type=MESH)
    pl.semaphore_wait(barrier, len(greeted) + 2 + 2 * inner)

    own_sends(KV, 0)
    run(mid, (own_sends, KV, 1))
    run(is2, (own_sends, Q, 1))
    run(end, (own_sends, Q, 0))
    x_near.start()
    x_far.start()
    each(share, KV + Q)
    x_near.wait()
    x_far.wait_recv()

    def norm():
        @pl.loop(0, T // 32)
        def _(i):
            at = rows(i, 32)
            wide = xa[at, :].astype(F32)
            scale = lax.rsqrt(jnp.mean(wide * wide, -1, keepdims=True) + 1e-6)
            xa[at, :] = (wide * scale * gain_ref[...].astype(F32)[None]).astype(BF)

    norm()
    run(last, (a3_send,))
    first(KV, 1)
    run(mid, (own_sends, Q, 0), (first, KV, 2))
    each(shared_wait, KV)
    project(KV, 0)

    def tables(plane, k):
        @pl.loop(0, 8)
        def _(i):
            at = rows(i, 128)
            place = plane * T + i * 128 + lax.broadcasted_iota(jnp.int32, (128, HEAD), 0)
            angle = place.astype(F32) * freq_ref[...][None]
            cos_ref[k, at, :] = jnp.cos(angle)
            sin_ref[k, at, :] = jnp.sin(angle) * jnp.where(lax.broadcasted_iota(jnp.int32, (128, HEAD), 1) < HALF, -1.0, 1.0)

    tables(z, 0)
    run(is2, (tables, 3, 1))
    run(end, (first, KV, 2))
    second(KV, 1)
    first(KV, 3)
    run(z == 1, (own_sends, Q, 1))
    run(mid, (relay, Q, 1))
    second(KV, 2)
    run(mid, (relay, QA, 2))
    second(KV, 3)
    run(mid, (xyforward, Q, 1), (relay, QB, 2))
    run(is2, (own_sends, OA, 1))
    project(KV, 1)
    project(KV, 2)
    run(end, (take, QA, 1))
    project(KV, 3)

    def make_kv():
        def one(g, k, v):
            ks[z, g] = turned(acc[:, k : k + HEAD])
            vs[z, g] = acc[:, v : v + HEAD].T.astype(BF)

        for g in range(3):
            one(g, g * HEAD, 384 + g * HEAD)
        run(low, (one, 3, 768, 896))

    make_kv()
    run(mid, (relay, Q, 3))
    kv_send(0)
    own_sends(O, 0)
    run(z == 1, (own_sends, O, 1))
    run(is2, (own_sends, OB, 1))
    run(end, (take, QB, 1))
    x_rest.start()
    for m in O:
        share(m)
        own_output(m).start()
    each(shared_wait, Q)
    project(Q, 0)
    run(end, (take, Q, 2))
    run(mid, (xyforward, Q, 2))
    second(Q, 1)
    run(end, (take, Q, 3))
    run(mid, (xyforward, Q, 3))
    project(Q, 1)
    second(Q, 2)
    run(is2, (kv_pass, 1))
    run(is2, (a3_pass,), (extra, 0), (extra, 1))
    second(Q, 3)
    run(z == 1, (relay, O, 1), (kv_pass, 1))
    project(Q, 2)
    run(is2, (extra, 2))
    run(z != 1, (first, O, 1))
    run(z == 1, (xyforward, O, 1))
    run(low, (first, O, 2))
    project(Q, 3)
    run(is2, (extra, 3))

    def ready(s, sem):
        pl.semaphore_signal(sem, device_id={"dp": dp, "sp": s}, device_id_type=MESH)

    run(last, (lambda: a3_out().wait_send(),), (ready, sp - 2, rdy3))
    ready(partner, rdy)

    def make_q():
        @pl.loop(0, heads)
        def _(g):
            for n in FOUR:
                q_s[g, pl.ds(n * T, T), :] = turned(acc[:, lanes(g * 4 + n, HEAD)])

    make_q()
    run(is2, (make_extra,), (first, O, 3))
    attend_own()
    second(O, 1)
    run(z < 2, (first, O, 3))
    pl.semaphore_wait(rdy, 1)

    def finish(g):
        for n in FOUR:
            at = pl.ds(n * T, T)
            xa[:, lanes(c * 16 + g * 4 + n, HEAD)] = mixed(g, at)
        seen_copy(g).start()

    whole = [(at, None) for at in range(0, QS, STRIP)]

    def attend():
        size = 2 * heads

        @pl.loop(6 - 6 * half * inner, 6 + z * size)
        def _(i):
            other = 1 - (i + 58) // 64
            k = i - 6 + size
            d, at = k // size, k % size
            head = other * 3 + (1 - other) * (at // 2)

            @pl.when(last & (at % 2 == 0))
            def _():
                run((d == 3) & (at == 0), (take, O, 2), (take, O, 3), (second, O, 2))
                run((d == 3) & (at == 4), (second, O, 3))
                kv_take(d, at // 2)
            run(is2 & (i == 4), (kv_pass, 2))

            block(other * (2 - i // 2) + (1 - other) * (z - d), head, head + other, lanes(i % 2, KB), whole, False)
            run(is2 & (i == 5), (finish_extra,), (second, O, 2))
            run(is2 & (i == 13), (second, O, 3))
            run((d == z) & (at % 2 == 1), (finish, at // 2))

    attend()

    def finish_all():
        pl.loop(0, 4)(finish)

    run(z == 0, (finish_all,))
    run(z < 2, (second, O, 2))
    run(last, (third, O, 1), (third, O, 2), (third, O, 3))
    swap = z // 3
    order = [o + swap * (p - o) for o, p in zip([z] + [origin(r) for r in ROUNDS], (2, 0, 3, 1))]

    def slot(m, i):
        return i % 2 * 2 + SLOT[m]

    def output_loads(m, i):
        return [pltpu.make_async_copy(bufs[m].at[2 * order[i] + j], wst.at[slot(m, i), pl.ds(j * H, H)], ld.at[slot(m, i), 0, j]) for j in TWO]

    def output_load(i):
        for m in O:
            for cp in output_loads(m, i):
                cp.start()

    def output(i):
        for m in O:
            for cp in output_loads(m, i):
                cp.wait()
            multiply(m, i, i % 2, lanes(order[i], T))

    def seen_wait(*gs):
        for g in gs:
            seen_in(g).wait_recv()

    for m in O:
        shared_wait(m)
        own_output(m).wait()
    output_load(0)
    run(low, (third, O, 1))
    output_load(1)
    seen_wait(*TWO)
    run(z == 1, (seen_wait, 2, 3))
    output(0)
    run(z != 1, (seen_wait, 2))
    run(z % 2 == 0, (seen_wait, 3))
    run(z < 2, (second, OA, 3))
    run(low, (third, O, 2))
    output_load(2)
    output(1)
    x_rest.wait_recv()
    rest_x = [cp for h in TWO for cp in (
        pltpu.make_async_copy(x_ref.at[:, lanes(c * 2 + h, W)], wst.at[2 + h, rows(c, H)], xl.at[1 + h]),
        pltpu.make_async_copy(xp_ref.at[:, pl.ds(h * W, W)], wst.at[2 + h, rows(oc, H)], xl.at[3 + h]))]
    for cp in rest_x:
        cp.start()
    run(z < 2, (second, OB, 3))
    run(last, (seen3_wait,), (seen_wait, 3))
    output(2)
    for cp in rest_x:
        cp.wait()

    def results(i):
        cols, to = pl.ds(i % 2 * 512, H), lanes(c * 4 + i, H)
        return (pltpu.make_async_copy(wst.at[2 + i // 2, rows(c, H), cols], y_ref.at[:, to], xl.at[5 + i]),
                remote(wst.at[2 + i // 2, rows(oc, H), cols], y_ref.at[:, to], ys.at[i], yr.at[i], dp, partner))

    def result_in(i):
        to = lanes((oc) * 4 + i, H)
        return remote(y_ref.at[:, to], y_ref.at[:, to], ys.at[i], yr.at[i], dp, partner)

    def last_loads(h):
        return [pltpu.make_async_copy(bufs[O[h]].at[2 * order[3] + j], wst.at[h, pl.ds(j * H, H)], ld.at[h, 0, j]) for j in TWO]

    for h in TWO:
        run(low, (third, (O[h],), 3))
        for cp in last_loads(h):
            cp.start()

    def final(h):
        depth, m = lanes(order[3], T), O[h]
        for cp in last_loads(h):
            cp.wait()
        for i in TWO:
            for n in TWO:
                cols = slice(i * 512 + n * 256, i * 512 + n * 256 + 256)
                for j in TWO:
                    at = pl.ds(j * H, H)
                    got = acc[at, h * W + cols.start : h * W + cols.stop] + _dot(xa[at, depth], wst[h, :, cols])
                    wst[2 + h, at, cols] = (wst[2 + h, at, cols].astype(F32) + got).astype(BF)
            for cp in results(2 * h + i):
                cp.start()

    final(0)
    final(1)

    for i in FOUR:
        near, far = results(i)
        near.wait()
        far.wait_send()
        result_in(i).wait_recv()
        seen_copy(i).wait_send()
    x_far.wait_send()
    x_rest.wait_send()
    def drain(m):
        here = bufs[m].at[sp]
        remote(here, here, ps.at[2 + m], pr.at[2 + m], dp, partner).wait_send()
        for r in ROUNDS:
            for k in FOUR:
                plane(m, r, k).wait_send()

    def sent(m, k):
        quarter = bufs[m].at[sp, rows(dp, QR)]
        for cc in TWO:
            remote(quarter, quarter, so.at[m, k, cc], zr.at[m, z, c], dp, (z + (inward, -inward)[k]) * 2 + cc).wait_send()

    def forwarded(m, r):
        for cc in TWO:
            zfwd(m, r, cc).wait_send()

    each(drain, KV + Q + O)
    for m in KV + Q + O:
        sent(m, 0)
        run(mid, (forwarded, m, 1))
        run(is1 if m in SHIP else mid, (sent, m, 1), (forwarded, m, 2), (forwarded, m, 3))

    def kv_sent(d, n):
        for cp in kv_out(d, n):
            cp.wait_send()

    run(z < 2, (kv_sent, 0, 4))
    run(z == 1, (kv_sent, 1, 4))

    def plane_two():
        for d in range(3):
            kv_sent(d, 3)
        a3_over(c).wait_send()
        for n in FOUR:
            seen3(n).wait_send()

    run(is2, (plane_two,))


def solution(mesh):
    def step(x, gain, wq, wk, wv, wo):
        freq = THETA ** (-(jnp.arange(HEAD) % (HALF)).astype(F32) / (HALF))
        far, near = pl.BlockSpec(memory_space=pl.ANY), pl.BlockSpec(memory_space=pltpu.VMEM)
        sems = pltpu.SemaphoreType.DMA
        y, *_ = pl.pallas_call(
            _layer,
            out_shape=[
                jax.ShapeDtypeStruct((H, D), BF),
                jax.ShapeDtypeStruct((H, C), BF),
                jax.ShapeDtypeStruct((T, D), BF),
                *(jax.ShapeDtypeStruct((8, H, n), BF) for n in WID),
            ],
            in_specs=[far, near, far, far, far, far, near],
            out_specs=[far] * 10,
            scratch_shapes=[
                pltpu.VMEM((T, D), BF),
                pltpu.VMEM((4, T, W), BF),
                pltpu.VMEM((T, C), F32),
                pltpu.VMEM((T, 768), F32),
                pltpu.VMEM((5, QS, HEAD), BF),
                pltpu.VMEM((4, 4, T, HEAD), BF),
                pltpu.VMEM((4, 4, HEAD, T), BF),
                pltpu.VMEM((5, HEAD + 8, QS), F32),
                pltpu.VMEM((5, 1, QS), F32),
                pltpu.VMEM((2, T, HEAD), F32),
                pltpu.VMEM((2, T, HEAD), F32),
                sems((7, 2, 2)),
                sems((7, 3, 2)),
                sems((7, 4, 2)),
                *[sems((7, 3, 4))] * 2,
                *[sems((3, 4, 2))] * 2,
                *[sems((9,))] * 2,
                *[sems((4,))] * 4,
                sems((4, 2, 3)),
                sems((12,)),
                *[sems((2,))] * 2,
                *[sems((4,))] * 2,
                *[pltpu.SemaphoreType.REGULAR] * 2,
            ],
            compiler_params=pltpu.CompilerParams(collective_id=0, has_side_effects=True, vmem_limit_bytes=63 * 2**20),
        )(x, gain, wq, wk, wv, wo, freq)
        return y

    tokens, whole = P(("dp", "sp")), P("sp")
    return jax.shard_map(
        step,
        mesh=mesh,
        in_specs=(tokens, P(), whole, whole, whole, whole),
        out_specs=tokens,
        check_vma=False,
    )
```
